32 devices in a mesh: seq: 8 (over z, x), chan: 2 (over y), dp: 2 (over core).
Axes of the slice: x: 2, y: 2, z: 4, core: 2. Of those that a mesh axis runs over, the one named last changes fastest.
Arguments:
- ssm_input: bfloat16 [2, 1024, 4096], P('dp', 'seq', 'chan'), may hold values from -6 to 6
- gate_z: bfloat16 [2, 1024, 4096], P('dp', 'seq', 'chan'), may hold values from -6 to 6
- b_proj: bfloat16 [2, 1024, 128], P('dp', 'seq'), may hold values from -0.52734375 to 0.52734375
- c_proj: bfloat16 [2, 1024, 128], P('dp', 'seq'), may hold values from -6 to 6
- step_size: float32 [2, 1024, 64], P('dp', 'seq', 'chan'), may hold values from 0.02 to 0.2
- log_decay: float32 [2, 1024, 64], P('dp', 'seq', 'chan'), may hold values from -1 to 0, as said below
- skip_d: float32 [64], P('chan'), may hold values from 0.5 to 1.5
- norm_gain: float32 [4096], P('chan'), may hold values from 0.5 to 1.5
- w_out: bfloat16 [4096, 2048], P('chan'), may hold values from -0.09375 to 0.09375
- d_out: bfloat16 [2, 1024, 2048], P('dp', 'seq', 'chan'), may hold values from -6 to 6
- game_lengths: int32 [2, 4], P('dp'), may hold values from 1 to 512, 1024 in all within a row
Outputs:
- out: bfloat16 [2, 1024, 2048], P('dp', 'seq', 'chan')
- grad_x: bfloat16 [2, 1024, 4096], P('dp', 'seq', 'chan')
- grad_gain: float32 [4096], P('chan')
- grad_skip: float32 [64], P('chan')
The draws below stay inside these ranges and needn't reach their ends.
Inputs may be any that keep to these rules, and one draw needn't show every extreme that they name: `game_lengths`: each row's 4 game lengths sum to 1024, and the longest is exactly 512. `log_decay`: a log decay per position and head.
All inputs are finite; a program needn't handle non-finite values.
Results may differ from the reference program's by a relative error of at most 0.017.
Values may be sent and summed in bfloat16 or wider, within the bound.
A program may use at most 64 MiB of HBM per device.

```python
import math
import jax
import jax.numpy as jnp
import numpy as np
from jax import lax

D = 2048
MIXER_HEADS = 64
HEADDIM = 64
DSTATE = 128
L_DEV = 128
GAMES = 4
BLOCK = 128
SEQUENCE_LENGTH = 1024
BATCH_SEQUENCES = 2


def draw_log_decay(key, part):
    random_keys = jax.random.split(jax.random.fold_in(key, 71), 7)
    fast_share = 0.5
    fast_pick = jax.random.uniform(random_keys[0], (BATCH_SEQUENCES, 1, MIXER_HEADS), jnp.float32) < fast_share
    fast_rate = jnp.exp(jax.random.uniform(random_keys[1], (BATCH_SEQUENCES, 1, MIXER_HEADS), jnp.float32, jnp.log(0.02), jnp.log(0.035)))
    slow_rate = jnp.exp(jax.random.uniform(random_keys[2], (BATCH_SEQUENCES, 1, MIXER_HEADS), jnp.float32, jnp.log(0.1 / SEQUENCE_LENGTH), jnp.log(0.7 / SEQUENCE_LENGTH)))
    baseline_rate = jnp.where(fast_pick, fast_rate, slow_rate)
    jaggedness = jnp.exp(jax.random.uniform(random_keys[3], (BATCH_SEQUENCES, SEQUENCE_LENGTH, MIXER_HEADS), jnp.float32, -0.7, 0.7))
    worker_level = jnp.exp(jax.random.uniform(random_keys[4], (BATCH_SEQUENCES, SEQUENCE_LENGTH // L_DEV, MIXER_HEADS), jnp.float32, -0.7, 0.7))
    worker_level = jnp.repeat(worker_level, L_DEV, axis=1)
    spike_places = jax.random.randint(random_keys[5], (BATCH_SEQUENCES, 3, MIXER_HEADS), 0, SEQUENCE_LENGTH)
    spike_depth = jax.random.uniform(random_keys[6], (BATCH_SEQUENCES, 3, MIXER_HEADS), jnp.float32, jnp.log(0.5), jnp.log(0.8))
    sequence_positions = jnp.arange(SEQUENCE_LENGTH, dtype=jnp.int32)
    spike_found = sequence_positions[None, :, None, None] == spike_places[:, None, :, :]
    spike_events = jnp.sum(jnp.where(spike_found, spike_depth[:, None, :, :], 0.0), axis=2)
    total = -baseline_rate * jaggedness * worker_level + spike_events
    return jnp.maximum(total, -1.0).astype(jnp.float32)


def shard_levels(key, dims, cuts, low, high):
    level = 1.0
    for dim, parts in cuts:
        draws = jax.random.uniform(jax.random.fold_in(jax.random.fold_in(key, 6), dim), (parts,), jnp.float32, low / len(cuts), high / len(cuts))
        level = level * jnp.repeat(jnp.exp(draws), dims[dim] // parts).reshape((-1,) + (1,) * (len(dims) - 1 - dim))
    return level


def profile(amount, total, reach, slope):
    loads = [(1 << 20) // math.isqrt(grade ** slope) + 1 for grade in range(2, amount + 1)]
    surplus, counts = total - reach - (amount - 1), [1] * (amount - 1)
    while surplus > 0:
        candidates = [i for i in range(amount - 1) if counts[i] < reach]
        pool, left = sum([loads[i] for i in candidates]), surplus
        for i in candidates:
            addition = min(reach - counts[i], max(1, left * loads[i] // pool), surplus)
            counts[i] = counts[i] + addition
            surplus = surplus - addition
    return np.array([reach] + counts)


def ragged(key, count, total, reach, lean):
    if count == 2:
        one = jax.random.randint(key, (), max(1, total - reach), min(reach, total - 1) + 1)
        return jnp.stack([one, total - one])
    tallies = jnp.asarray(profile(count, total, reach, lean), jnp.int32)
    twos = (count - 1) // 2
    source_of, receiver = tallies[1:1 + 2 * twos:2], tallies[2:2 + 2 * twos:2]
    slack = jnp.minimum(source_of - 1, reach - receiver)
    passed = jax.random.randint(jax.random.fold_in(key, 1), (twos,), 0, 1 << 20) % (slack + 1)
    tallies = tallies.at[1:1 + 2 * twos:2].set(source_of - passed).at[2:2 + 2 * twos:2].set(receiver + passed)
    return tallies[jax.random.permutation(jax.random.fold_in(key, 2), count)]


def normal_values(rng, extent, deviation, bound, cuts=(), kind=jnp.bfloat16):
    gain = shard_levels(rng, extent, cuts, -0.22, 0.18) if cuts else 1.0
    entries = jax.random.normal(rng, extent, jnp.float32) * deviation * gain
    return jnp.minimum(jnp.maximum(entries, -bound), bound).astype(kind)


def setup_inputs(seed: int = 0) -> dict:
    seeds = jax.random.split(jax.random.key(seed), 12)
    ssm_input = normal_values(seeds[0], (BATCH_SEQUENCES, SEQUENCE_LENGTH, MIXER_HEADS * HEADDIM), 1.0, 6.0, ((0, 2), (1, 8), (2, 2)))
    gate_z = normal_values(seeds[1], (BATCH_SEQUENCES, SEQUENCE_LENGTH, MIXER_HEADS * HEADDIM), 1.0, 6.0, ((0, 2), (1, 8), (2, 2)))
    b_proj = normal_values(seeds[2], (BATCH_SEQUENCES, SEQUENCE_LENGTH, DSTATE), (DSTATE ** -0.5), 0.52734375, ((0, 2), (1, 8)))
    c_proj = normal_values(seeds[3], (BATCH_SEQUENCES, SEQUENCE_LENGTH, DSTATE), 1.0, 6.0, ((0, 2), (1, 8)))
    step_size = jnp.clip(jnp.exp(math.log(0.2) - 2.3025851 * jax.random.uniform(seeds[4], (BATCH_SEQUENCES, SEQUENCE_LENGTH, MIXER_HEADS), jnp.float32) ** shard_levels(seeds[4], (BATCH_SEQUENCES, SEQUENCE_LENGTH, MIXER_HEADS), ((0, 2), (1, 8), (2, 2)), -0.2, 0.2)), 0.02, 0.2)
    log_decay = draw_log_decay(jax.random.fold_in(seeds[11], 71), 0)
    skip_d = jnp.clip(0.5 + 1.0 * jax.random.uniform(seeds[6], (MIXER_HEADS,), jnp.float32) ** shard_levels(seeds[6], (MIXER_HEADS,), ((0, 2),), -0.2, 0.2), 0.5, 1.5)
    norm_gain = jnp.clip(1.0 + 0.1 * jax.random.normal(seeds[7], (MIXER_HEADS * HEADDIM,), jnp.float32), 0.5, 1.5)
    w_out = normal_values(seeds[8], (MIXER_HEADS * HEADDIM, D), (MIXER_HEADS * HEADDIM) ** -0.5, 0.09375, ((0, 2),))
    d_out = normal_values(seeds[9], (BATCH_SEQUENCES, SEQUENCE_LENGTH, D), 1.0, 6.0, ((0, 2), (1, 8), (2, 2)))
    game_lengths = jax.vmap(lambda own: ragged(own, GAMES, SEQUENCE_LENGTH, SEQUENCE_LENGTH // 2, 2))(jax.random.split(seeds[10], BATCH_SEQUENCES)).reshape((BATCH_SEQUENCES, GAMES)).astype(jnp.int32)
    return dict(ssm_input=ssm_input, gate_z=gate_z, b_proj=b_proj, c_proj=c_proj, step_size=step_size, log_decay=log_decay, skip_d=skip_d, norm_gain=norm_gain, w_out=w_out, d_out=d_out, game_lengths=game_lengths)


NORM_EPS = 1e-05
PRECISE = lax.Precision.HIGHEST

def block_parts(c_block, b_block, dt_block, decay_block, reset_block):
    block_len = c_block.shape[0]
    running = jnp.cumsum(decay_block, axis=0)
    reset_count = jnp.cumsum(reset_block, axis=0).astype(jnp.int32)
    scores = jnp.dot(c_block, b_block.T, preferred_element_type=jnp.float32)
    indices = jnp.arange(block_len, dtype=jnp.int32)
    allowed = (indices[:, None] >= indices[None, :]) & (reset_count[:, None] == reset_count[None, :])
    log_gap = running.T[:, :, None] - running.T[:, None, :]
    mixing = jnp.where(allowed[None], jnp.exp(jnp.minimum(log_gap, 0.0)), 0.0) * scores[None] * dt_block.T[:, None, :]
    mixing = mixing.astype(jnp.bfloat16)
    end_count = reset_count[-1]
    carry_weight = jnp.where((reset_count == 0)[:, None], jnp.exp(running), 0.0)
    tail_weight = jnp.where((reset_count == end_count)[:, None], jnp.exp(running[-1][None, :] - running), 0.0)
    block_decay = jnp.where(end_count == 0, jnp.exp(running[-1]), 0.0)
    return (mixing, carry_weight, tail_weight, block_decay)

def one_sequence(ssm_input, gate_z, b_proj, c_proj, step_size, log_decay, starts, skip_d, norm_gain, w_out, d_out):
    sequence_positions = jnp.arange(SEQUENCE_LENGTH, dtype=jnp.int32)
    resets = jnp.any(sequence_positions[:, None] == starts[None, :], axis=1).astype(jnp.int32)
    count_blocks = SEQUENCE_LENGTH // BLOCK

    def blocked(array):
        return array.reshape((count_blocks, BLOCK) + array.shape[1:])
    x_heads = ssm_input.reshape(SEQUENCE_LENGTH, MIXER_HEADS, HEADDIM)
    zero_state = jnp.zeros((MIXER_HEADS, DSTATE, HEADDIM), jnp.float32)

    def forward_step(state, block_inputs):
        x_block, c_block, b_block, dt_block, decay_block, reset_block = block_inputs
        mixing, carry_weight, tail_weight, block_decay = block_parts(c_block, b_block, dt_block, decay_block, reset_block)
        inside = jnp.einsum('hts,shp->thp', mixing.astype(jnp.float32), x_block.astype(jnp.float32))
        carried = carry_weight[:, :, None] * jnp.einsum('tn,hnp->thp', c_block.astype(jnp.float32), state, precision=PRECISE)
        scaled = ((tail_weight * dt_block)[:, :, None] * x_block.astype(jnp.float32)).astype(jnp.bfloat16)
        fresh_state = jnp.einsum('sn,shp->hnp', b_block.astype(jnp.float32), scaled.astype(jnp.float32))
        return (block_decay[:, None, None] * state + fresh_state, inside + carried)
    _, ssd_blocks = lax.scan(forward_step, zero_state, (blocked(x_heads), blocked(c_proj), blocked(b_proj), blocked(step_size), blocked(log_decay), blocked(resets)))
    ssd_out = ssd_blocks.reshape(SEQUENCE_LENGTH, MIXER_HEADS, HEADDIM) + skip_d[None, :, None] * x_heads.astype(jnp.float32)
    gate_act = jax.nn.silu(gate_z.astype(jnp.float32))
    gated = ssd_out.reshape(SEQUENCE_LENGTH, MIXER_HEADS * HEADDIM) * gate_act
    inv_rms = lax.rsqrt(lax.optimization_barrier(jnp.mean(gated * gated, axis=1)) + NORM_EPS)
    normed = (gated * norm_gain).astype(jnp.bfloat16)
    projected = jnp.dot(normed, w_out, preferred_element_type=jnp.float32)
    out = (inv_rms[:, None] * projected).astype(jnp.bfloat16)
    pulled = jnp.dot(d_out, w_out.T, preferred_element_type=jnp.float32)
    out_dot = lax.optimization_barrier(jnp.sum(d_out.astype(jnp.float32) * projected, axis=1))
    d_normed = inv_rms[:, None] * pulled
    gain_part = lax.optimization_barrier(jnp.sum(gated * d_normed, axis=0))
    d_ssd = ((norm_gain * d_normed - (inv_rms ** 3 * out_dot / (MIXER_HEADS * HEADDIM))[:, None] * gated) * gate_act).astype(jnp.bfloat16)
    d_heads = d_ssd.reshape(SEQUENCE_LENGTH, MIXER_HEADS, HEADDIM)
    skip_part = lax.optimization_barrier(jnp.sum(d_heads.astype(jnp.float32) * x_heads.astype(jnp.float32), axis=(0, 2)))

    def backward_step(adjoint, block_inputs):
        d_block, c_block, b_block, dt_block, decay_block, reset_block = block_inputs
        mixing, carry_weight, tail_weight, block_decay = block_parts(c_block, b_block, dt_block, decay_block, reset_block)
        inside = jnp.einsum('hts,thp->shp', mixing.astype(jnp.float32), d_block.astype(jnp.float32))
        carried = (dt_block * tail_weight)[:, :, None] * jnp.einsum('sn,hnp->shp', b_block.astype(jnp.float32), adjoint, precision=PRECISE)
        weighted = (carry_weight[:, :, None] * d_block.astype(jnp.float32)).astype(jnp.bfloat16)
        fresh_adjoint = jnp.einsum('tn,thp->hnp', c_block.astype(jnp.float32), weighted.astype(jnp.float32))
        return (fresh_adjoint + block_decay[:, None, None] * adjoint, inside + carried)
    _, grad_blocks = lax.scan(backward_step, zero_state, (blocked(d_heads), blocked(c_proj), blocked(b_proj), blocked(step_size), blocked(log_decay), blocked(resets)), reverse=True)
    grad_heads = grad_blocks.reshape(SEQUENCE_LENGTH, MIXER_HEADS, HEADDIM) + skip_d[None, :, None] * d_heads.astype(jnp.float32)
    grad_x = grad_heads.astype(jnp.bfloat16).reshape(SEQUENCE_LENGTH, MIXER_HEADS * HEADDIM)
    return (out, grad_x, gain_part, skip_part)

def reference(ssm_input, gate_z, b_proj, c_proj, step_size, log_decay, skip_d, norm_gain, w_out, d_out, game_lengths):
    outs_list = []
    grads_list = []
    gain_total = jnp.zeros((MIXER_HEADS * HEADDIM,), jnp.float32)
    skip_total = jnp.zeros((MIXER_HEADS,), jnp.float32)
    for index in range(BATCH_SEQUENCES):
        lengths = game_lengths[index].astype(jnp.int32)
        starts = (jnp.cumsum(lengths) - lengths).astype(jnp.int32)
        out, grad_x, gain_part, skip_part = one_sequence(ssm_input[index], gate_z[index], b_proj[index], c_proj[index], step_size[index], log_decay[index], starts, skip_d, norm_gain, w_out, d_out[index])
        outs_list.append(out)
        grads_list.append(grad_x)
        gain_total = gain_total + gain_part
        skip_total = skip_total + skip_part
    return (jnp.stack(outs_list), jnp.stack(grads_list), gain_total, skip_total)
```

```python
import functools
import types

import jax
import jax.numpy as jnp
from jax import lax
from jax.experimental import pallas as pl
from jax.experimental.pallas import tpu as pltpu
from jax.sharding import PartitionSpec as P

NORM_EPS = 1e-05
F32 = jnp.float32
BF16 = jnp.bfloat16
MESH = pl.DeviceIdType.MESH
FWD, BWD = 0, 1


def dot(a, b):
    return lax.dot_general(a, b, (((1,), (0,)), ((), ())), preferred_element_type=F32)


def dot_rows(a, b):
    return lax.dot_general(a, b, (((0,), (0,)), ((), ())), preferred_element_type=F32)


def dot_cols(a, b):
    return lax.dot_general(a, b, (((1,), (1,)), ((), ())), preferred_element_type=F32)


def split(value, terms):
    parts = []
    for _ in range(terms):
        part = value.astype(BF16)
        parts.append(part)
        value = value - part.astype(F32)
    return parts


def kernel(sizes, names, *refs):
    r = types.SimpleNamespace(**dict(zip(names, refs)))
    n_seq, n_chan, n_dp, heads, games, chunks, group = sizes
    rows, width = r.x.shape
    hd = width // heads
    half = width // 2
    hh = heads // 2
    cw = half // chunks
    gw = group * cw
    groups = chunks // group
    total_width = width * n_chan
    nb = r.out.shape[1]
    seq = lax.axis_index("seq")
    chan = lax.axis_index("chan")
    dp = lax.axis_index("dp")
    mine = lax.rem(seq, 2)
    other = 1 - mine
    pair = seq + 1 - 2 * mine
    partner = {"seq": pair}
    place = seq // 2
    last = n_seq // 2 - 1
    has_prev, has_next = place > 0, place < last
    prev_dev = {"seq": lax.rem(seq + n_seq - 2, n_seq)}
    next_dev = {"seq": lax.rem(seq + 2, n_seq)}

    siblings = [{"dp": lax.rem(dp + k, n_dp)} for k in range(1, n_dp)]
    offs = [lax.rem(chan + off, n_chan) for off in range(1, n_chan)]
    chan_peers = [{"chan": o} for o in offs]
    stat_peers = [partner] + chan_peers + [{"seq": pair, "chan": o} for o in offs]
    greet = [partner] + chan_peers + siblings
    barrier = pltpu.get_barrier_semaphore()

    def hello(peer):
        pl.semaphore_signal(barrier, inc=1, device_id=peer, device_id_type=MESH)

    for peer in greet:
        hello(peer)
    pl.when(has_prev)(lambda: hello(prev_dev))
    pl.when(has_next)(lambda: hello(next_dev))

    my_half = pl.ds(pl.multiple_of(mine * half, half), half)
    other_half = pl.ds(pl.multiple_of(other * half, half), half)
    order = {}

    def load(name, src, dst):
        order[name] = pltpu.make_async_copy(src, dst, r.load_sem.at[len(order)])
        order[name].start()

    def load_chunks(name, which, dst):
        for c in range(chunks):
            at = pl.ds(pl.multiple_of(which * half + c * cw, cw), cw)
            pltpu.make_async_copy(r.x.at[:, at], dst.at[c], r.load_sem.at[len(order)]).start()
        order[name] = pltpu.make_async_copy(dst, dst, r.load_sem.at[len(order)])

    load("ld", r.ld, r.ldv)
    load("gl", r.gl, r.gls)
    load("dt", r.dt, r.smf.at[1])
    load("b", r.b, r.bv.at[mine])
    load_chunks("xo", other, r.xo)
    load("do", r.do, r.dfull.at[0])
    load_chunks("x", mine, r.xv.at[mine])
    load("c", r.c, r.cv.at[mine])
    load("skip", r.skip, r.skipv)
    load("zo", r.z.at[:, other_half], r.zo)
    load("z", r.z.at[:, my_half], r.zv.at[mine])
    load("gain", r.gain, r.gainv)
    load("w", r.w, r.wv)

    def remote(src, dst, ssem, rsem, peer):
        return pltpu.make_async_remote_copy(
            src_ref=src, dst_ref=dst, send_sem=ssem, recv_sem=rsem, device_id=peer, device_id_type=MESH
        )

    def ccols(c):
        return pl.ds(pl.multiple_of(c * cw, cw), cw)

    def gcols(g):
        return pl.ds(pl.multiple_of(g * gw, gw), gw)

    def gain_of(g):
        return r.gainv[:, pl.ds(pl.multiple_of(mine * half + g * gw, gw), gw)]

    def send_sm(blk):
        src = r.smf.at[:, pl.ds(pl.multiple_of(other * hh, hh), hh), :]
        return remote(src, r.sm.at[blk], r.p_send.at[0], r.p_recv.at[0], partner)

    def send_b(blk):
        return remote(r.bv.at[blk], r.bv.at[blk], r.p_send.at[1], r.p_recv.at[1], partner)

    def send_c(blk):
        return remote(r.cv.at[blk], r.cv.at[blk], r.p_send.at[2], r.p_recv.at[2], partner)

    def send_z(blk):
        return remote(r.zo, r.zv.at[blk], r.p_send.at[3], r.p_recv.at[3], partner)

    def send_n():
        return remote(r.nrm.at[other], r.nrx, r.p_send.at[4], r.p_recv.at[4], partner)

    def send_x(blk, c):
        return remote(r.xo.at[c], r.xv.at[blk, c], r.x_send, r.x_recv.at[c], partner)

    def send_p(blk, g):
        return remote(r.ptx.at[g], r.pv.at[blk, g], r.pl_send, r.pl_recv.at[g], partner)

    def send_g(c, of):
        at = pl.ds(pl.multiple_of(of * half + c * cw, cw), cw)
        return remote(r.gtx.at[c], r.gx.at[:, at], r.g_send, r.g_recv.at[c], partner)

    def send_chain(d, c):
        to = next_dev if d == FWD else prev_dev
        return remote(r.txc.at[d, c], r.st.at[d, d, c], r.c_send.at[d], r.c_recv.at[d, c], to)

    do_copies = [
        remote(r.dfull.at[0], r.dfull.at[k + 1], r.do_send.at[k], r.do_recv.at[k], peer)
        for k, peer in enumerate(chan_peers)
    ]

    row_i = lax.broadcasted_iota(jnp.int32, (rows, rows), 0)
    col_i = lax.broadcasted_iota(jnp.int32, (rows, rows), 1)
    causal = row_i >= col_i
    tri = causal.astype(F32).astype(BF16)
    spread = (
        lax.broadcasted_iota(jnp.int32, (hh, half), 1) // hd == lax.broadcasted_iota(jnp.int32, (hh, half), 0)
    ).astype(F32).astype(BF16)

    def spread_all(which):
        at = lax.broadcasted_iota(jnp.int32, (heads, half), 1) // hd + which * hh
        return (at == lax.broadcasted_iota(jnp.int32, (heads, half), 0)).astype(F32).astype(BF16)

    order["ld"].wait()
    running = jnp.zeros((heads, rows), F32)
    for part in split(r.ldv[...], 3):
        running = running + dot_cols(part, tri)
    r.smf[0] = running
    order["gl"].wait()

    def counts(blk):
        base = (2 * place + blk) * rows
        col = jnp.zeros((rows, 1), jnp.int32)
        row = jnp.zeros((1, rows), jnp.int32)
        end = jnp.zeros((1, 1), jnp.int32)
        pos_col = base + lax.broadcasted_iota(jnp.int32, (rows, 1), 0)
        pos_row = base + lax.broadcasted_iota(jnp.int32, (1, rows), 1)
        pos_end = base + rows - 1 + lax.broadcasted_iota(jnp.int32, (1, 1), 0)
        begin = jnp.int32(0)
        for g in range(games):
            here = (begin >= base).astype(jnp.int32)
            col = col + (pos_col >= begin).astype(jnp.int32) * here
            row = row + (pos_row >= begin).astype(jnp.int32) * here
            end = end + (pos_end >= begin).astype(jnp.int32) * here
            begin = begin + r.gls[0, g]
        return col, row, end

    def expand(value, terms):
        total = None
        for part in split(value, terms):
            piece = dot_rows(part, spread)
            total = piece if total is None else total + piece
        return total

    def prepare(blk):
        run = r.sm[blk, 0]
        _, row, end = counts(blk)
        carry = jnp.where(row == 0, jnp.exp(run), 0.0)
        tail = jnp.where(row == end, jnp.exp(run[:, rows - 1 : rows] - run), 0.0)
        r.tdt_e[blk] = expand(tail * r.sm[blk, 1], 2)
        r.carry_e[blk] = expand(carry, 2)
        r.runc[blk] = run.T
        r.bt[blk] = r.bv[blk].T

    my_heads = pl.ds(pl.multiple_of(mine * hh, hh), hh)
    order["dt"].wait()
    r.sm[mine] = r.smf[:, my_heads, :]
    order["b"].wait()
    prepare(mine)

    def report():
        pl.semaphore_signal(r.up, inc=1, device_id=prev_dev, device_id_type=MESH)

    def relay():
        pl.semaphore_wait(r.up, 1)
        pl.when(has_prev)(report)

    static = len(greet)
    pl.semaphore_wait(barrier, static + has_prev.astype(jnp.int32) + has_next.astype(jnp.int32))
    pl.when(place == last)(report)
    order["xo"].wait()
    order["do"].wait()
    order["c"].wait()
    order["zo"].wait()

    def first_sends():
        send_sm(mine).start()
        send_b(mine).start()
        for c in range(chunks):
            send_x(mine, c).start()
        send_c(mine).start()

    def cotangent_sends():
        for copy in do_copies:
            copy.start()

    def lead_sends():
        first_sends()
        cotangent_sends()

    def gate_sends():
        send_z(mine).start()

    pl.when(dp == 0)(lead_sends)
    pl.when((dp == 0) & (place >= last - 1))(gate_sends)
    order["x"].wait()

    def x_group(blk, g):
        return jnp.concatenate([r.xv[blk, g * group + k] for k in range(group)], axis=1).astype(F32)


    def fresh(blk, g):
        cols = gcols(g)
        scaled = (r.tdt_e[blk, :, cols] * x_group(blk, g)).astype(BF16)
        block = dot(r.bt[blk], scaled)
        for k in range(group):
            r.f[blk, g * group + k] = block[:, k * cw : (k + 1) * cw]

    def loop(n, body):
        def step(i, _):
            body(i)
            return 0

        lax.fori_loop(0, n, step, 0)

    loop(groups, lambda g: fresh(mine, g))
    order["skip"].wait()
    skip_pad = jnp.concatenate([r.skipv[...], jnp.zeros((7, heads), F32)], axis=0)
    skip_rows = None
    for part in split(skip_pad, 3):
        piece = dot(part, spread_all(mine))
        skip_rows = piece if skip_rows is None else skip_rows + piece
    r.skip_e[...] = skip_rows[0:1, :]
    pos_lane = lax.broadcasted_iota(jnp.int32, (rows, 2 * hd), 1) < hd

    def block_diag(two):
        two = two.astype(F32)
        return jnp.concatenate(
            [jnp.where(pos_lane, two, 0.0), jnp.where(pos_lane, 0.0, two)], axis=0
        ).astype(BF16)

    def intra(blk):
        col, row, _ = counts(blk)
        r.ct[blk] = r.cv[blk].T
        scores = jnp.where(causal & (col == row), dot_cols(r.cv[blk], r.bv[blk]), 0.0)
        for q in range(hh // 2):
            cols = slice(q * 2 * hd, (q + 1) * 2 * hd)
            mixes = []
            for h in (2 * q, 2 * q + 1):
                gap = jnp.minimum(r.runc[blk, :, h : h + 1] - r.sm[blk, 0, h : h + 1, :], 0.0)
                mixes.append((jnp.exp(gap) * scores * r.sm[blk, 1, h : h + 1, :]).astype(BF16))
                r.mix[blk, q, (h % 2) * rows : (h % 2 + 1) * rows, :] = mixes[-1]
            at = q * 2 * hd
            two = r.xv[blk, at // cw, :, at % cw : at % cw + 2 * hd]
            r.inside[blk, :, cols] = dot(jnp.concatenate(mixes, axis=1), block_diag(two)) + r.skip_e[
                :, cols
            ] * two.astype(F32)

    def silu(blk):
        def body(g):
            zf = r.zv[blk, :, gcols(g)].astype(F32)
            r.act[blk, :, gcols(g)] = zf / (1.0 + jnp.exp(-zf))

        loop(groups, body)

    def chain(d, c):
        enters = has_prev if d == FWD else has_next
        leaves = has_next if d == FWD else has_prev

        @pl.when(enters)
        def _():
            send_chain(d, c).wait_recv()

        @pl.when(jnp.logical_not(enters))
        def _():
            r.st[d, d, c] = jnp.zeros((r.st.shape[3], cw), BF16)

        one, two = (0, 1) if d == FWD else (1, 0)
        mid = r.carry_e[one, rows - 1 : rows, ccols(c)] * r.st[d, d, c].astype(F32) + r.f[one, c]
        r.st[d, 1 - d, c] = mid.astype(BF16)

        @pl.when(leaves)
        def _():
            r.txc[d, c] = (r.carry_e[two, rows - 1 : rows, ccols(c)] * mid + r.f[two, c]).astype(BF16)
            send_chain(d, c).start()

    def meet(g):
        for k in range(group):
            send_x(other, g * group + k).wait_recv()
        fresh(other, g)

    def partner_arrives():
        send_sm(other).wait_recv()
        send_b(other).wait_recv()

    def chain_group(d, g):
        for k in range(group):
            chain(d, g * group + k)

    def meet_chain(g):
        meet(g)
        chain_group(FWD, g)

    def own_local():
        intra(mine)
        order["z"].wait()
        silu(mine)

    def late_sends():
        own_local()
        pl.semaphore_wait(r.go, 1)
        lead_sends()
        pl.when(place >= last - 1)(gate_sends)

    def lead_done():
        for k in range(1, n_dp):
            pl.semaphore_signal(r.go, inc=1, device_id={"dp": k}, device_id_type=MESH)

    pl.when(dp > 0)(late_sends)
    partner_arrives()
    pl.when((dp == 0) & (place < last - 1))(lead_done)
    prepare(other)
    pl.when(place == last - 1)(relay)

    def pull(lo, hi):
        def body(i, _):
            which = jnp.where(i < groups, other, mine)
            g = lax.rem(i, groups)
            feats = pl.ds(pl.multiple_of(which * half + g * gw, gw), gw)
            total = None
            for k in range(n_chan):
                source = lax.rem(chan + n_chan - k, n_chan)
                piece = dot_cols(r.dfull[k], r.wv[feats, pl.ds(pl.multiple_of(source * nb, nb), nb)])
                total = piece if total is None else total + piece
            value = total.astype(BF16)

            @pl.when(i < groups)
            def _():
                r.ptx[g] = value
                send_p(mine, g).start()

            @pl.when(i >= groups)
            def _():
                r.pv[mine, g] = value

            return 0

        lax.fori_loop(lo, hi, body, 0)

    def pull_ready():
        order["w"].wait()
        for copy in do_copies:
            copy.wait_recv()

    tiles = 2 * groups
    late_place = place >= last - 1

    def pull_first():
        pl.when(dp == 0)(own_local)
        pull_ready()
        pull(0, groups)
        pl.when(dp == 0)(lead_done)

    pl.when(late_place)(pull_first)
    pl.when(place == 0)(lambda: loop(groups, meet_chain))
    pl.when(place > 0)(lambda: loop(groups, meet))
    pl.when((place > 0) & (place < last - 1))(relay)
    pl.when((dp == 0) & (place < last - 1))(own_local)
    send_c(other).wait_recv()
    intra(other)
    pl.when(place < last - 1)(gate_sends)
    pl.when(place == last)(lambda: pull(groups, tiles))
    order["gain"].wait()
    r.sums[...] = jnp.zeros(r.sums.shape, F32)

    def gate(g):
        cols = gcols(g)
        send_p(other, g).wait_recv()
        for blk in (0, 1):
            carried = jnp.concatenate(
                [dot(r.cv[blk], r.st[FWD, blk, g * group + k]) for k in range(group)], axis=1
            )
            gated = (r.inside[blk, :, cols] + r.carry_e[blk, :, cols] * carried) * r.act[blk, :, cols]
            normed = (gated * gain_of(g)).astype(BF16)
            r.gated[blk, :, cols] = gated
            r.nrm[blk, :, cols] = normed
            sq = gated * gated
            od = normed.astype(F32) * r.pv[blk, g].astype(F32)
            squares, dots = r.sums[blk, 0], r.sums[blk, 1]
            for k in range(gw // 128):
                squares = squares + sq[:, k * 128 : (k + 1) * 128]
                dots = dots + od[:, k * 128 : (k + 1) * 128]
            r.sums[blk, 0] = squares
            r.sums[blk, 1] = dots

    def gate_ready():
        send_z(other).wait_recv()
        silu(other)

    def chain_gate(g):
        chain_group(FWD, g)
        gate(g)

    def at_last():
        gate_ready()
        loop(groups, chain_gate)

    def before_last():
        pl.when(place > 0)(lambda: loop(chunks, lambda c: chain(FWD, c)))
        pl.when(place < last - 1)(pull_ready)
        pull(jnp.where(place == last - 1, groups, 0), tiles)
        gate_ready()
        loop(groups, gate)

    pl.when(place == last)(at_last)
    pl.when(place < last)(before_last)

    lane = lax.broadcasted_iota(jnp.int32, (rows, 128), 1)
    stats = jnp.zeros((rows, 128), F32)
    for blk in (0, 1):
        for k in (0, 1):
            col = jnp.sum(r.sums[blk, k], axis=1, keepdims=True)
            stats = jnp.where(lane == 2 * blk + k, col, stats)
    r.stat_tx[...] = stats.T[0:8, :]
    st_copies = []
    for k, peer in enumerate(stat_peers):
        st_copies.append(remote(r.stat_tx, r.stat_rx.at[k], r.st_send, r.st_recv.at[k], peer))
        st_copies[-1].start()
    pl.when(place < last - 1)(lambda: send_n().start())
    total = r.stat_tx[...]
    for k, copy in enumerate(st_copies):
        copy.wait_recv()
        total = total + r.stat_rx[k]
    stat_cols = jnp.concatenate([total, jnp.zeros((rows - 8, rows), F32)], axis=0).T
    inv, back = [], []
    for blk in (0, 1):
        inv.append(lax.rsqrt(stat_cols[:, 2 * blk : 2 * blk + 1] / total_width + NORM_EPS))
        back.append(inv[blk] * inv[blk] * inv[blk] * stat_cols[:, 2 * blk + 1 : 2 * blk + 2] / total_width)
        r.invs[blk] = jnp.broadcast_to(inv[blk], (rows, 128))
        r.backs[blk] = jnp.broadcast_to(back[blk], (rows, 128))

    def wide(ref, blk):
        return jnp.concatenate([ref[blk]] * (gw // 128), axis=1)

    def cotangent(g):
        cols = gcols(g)
        for blk in (0, 1):
            gated = r.gated[blk, :, cols]
            d_normed = wide(r.invs, blk) * r.pv[blk, g].astype(F32)
            d = ((gain_of(g) * d_normed - wide(r.backs, blk) * gated) * r.act[blk, :, cols]).astype(BF16)
            r.d[blk, :, cols] = d
            weighted = (r.carry_e[blk, :, cols] * d.astype(F32)).astype(BF16)
            block = dot(r.ct[blk], weighted)
            for k in range(group):
                r.f[blk, g * group + k] = block[:, k * cw : (k + 1) * cw]

    def cotangent_chain(g):
        cotangent(g)
        chain_group(BWD, g)

    pl.when(place == last)(lambda: loop(groups, cotangent_chain))
    pl.when(place < last)(lambda: loop(groups, cotangent))

    def terms(g):
        cols = gcols(g)
        gain_sum = skip_sum = None
        for blk in (0, 1):
            a = r.gated[blk, :, cols] * (wide(r.invs, blk) * r.pv[blk, g].astype(F32))
            s = r.d[blk, :, cols].astype(F32) * x_group(blk, g)
            gain_sum = a if gain_sum is None else gain_sum + a
            skip_sum = s if skip_sum is None else skip_sum + s
        r.red_tx[0, 0:1, cols] = jnp.sum(gain_sum, axis=0, keepdims=True)
        r.red_tx[0, 1:2, cols] = jnp.sum(skip_sum, axis=0, keepdims=True)

    loop(groups, terms)

    root = n_dp - 1

    def red_root(k):
        to = {"dp": root}
        return remote(r.red_tx.at[0], r.red_rx.at[k], r.rd_send.at[0], r.rd_recv.at[k], to)

    everyone = [
        {"seq": lax.rem(seq + k, n_seq), "dp": lax.rem(dp + j, n_dp)}
        for k in range(n_seq)
        for j in range(n_dp)
        if (k, j) != (0, 0)
    ]

    def red_all(which, k):
        return remote(r.red_tx.at[1], r.fin.at[which], r.fin_send, r.fin_recv, everyone[k])

    for k in range(root):
        pl.when(dp == k)(red_root(k).start)

    def spread_sums():
        total = r.red_tx[0]
        for k in range(root):
            red_root(k).wait_recv()
            total = total + r.red_rx[k]
        r.red_tx[1] = total
        r.fin[seq] = total
        for k in range(len(everyone)):
            red_all(seq, k).start()


    def intra_back(blk):
        for q in range(hh // 2):
            cols = slice(q * 2 * hd, (q + 1) * 2 * hd)
            two = r.d[blk, :, cols]
            r.inside[blk, :, cols] = dot_rows(r.mix[blk, q], block_diag(two)) + r.skip_e[:, cols] * two.astype(
                F32
            )

    intra_back(other)
    intra_back(mine)
    pl.when(late_place)(lambda: send_n().start())
    pl.when(place == 0)(relay)
    pl.when(dp == root)(spread_sums)

    tile_n = min(256, nb)
    per = nb // tile_n
    sent_tiles = (n_chan - 1) * per

    def pj(t):
        to = {"chan": lax.rem(chan + 1 + t // per, n_chan)}
        return remote(r.proj_tx.at[t], r.proj_rx.at[t], r.pj_send, r.pj_recv.at[t], to)

    def project(t):
        block = lax.rem(chan + 1 + t // per, n_chan)
        at = pl.ds(pl.multiple_of(block * nb + lax.rem(t, per) * tile_n, tile_n), tile_n)
        value = dot(r.nrm[mine], r.wv[my_half, at]) + dot(r.nrx[...], r.wv[other_half, at])

        @pl.when(t < sent_tiles)
        def _():
            r.proj_tx[t] = value.astype(BF16)
            pj(t).start()

        @pl.when(t >= sent_tiles)
        def _():
            r.proj_own[t - sent_tiles] = value

    n_tiles = sent_tiles + per

    def finish(c):
        cols = ccols(c)

        def value(blk):
            carried = dot(r.bv[blk], r.st[BWD, blk, c])
            return (r.inside[blk, :, cols] + r.tdt_e[blk, :, cols] * carried).astype(BF16)

        r.gtx[c] = value(other)
        send_g(c, mine).start()
        r.gx[:, pl.ds(pl.multiple_of(mine * half + c * cw, cw), cw)] = value(mine)

    def chain_finish(c):
        chain(BWD, c)
        finish(c)

    def back_first():
        send_n().wait_recv()
        loop(sent_tiles, project)
        loop(chunks, chain_finish)
        loop(per, lambda t: project(sent_tiles + t))

    def back_middle():
        loop(chunks, lambda c: chain(BWD, c))
        loop(chunks, finish)
        send_n().wait_recv()
        loop(n_tiles, project)

    def back_last():
        loop(chunks, finish)
        send_n().wait_recv()
        loop(n_tiles, project)

    pl.when(place == 0)(back_first)
    pl.when((place > 0) & (place < last))(back_middle)
    pl.when(place == last)(back_last)
    inv_mine = jnp.concatenate([r.invs[mine]] * (tile_n // 128), axis=1)
    for i in range(per):
        value = r.proj_own[i]
        for k in range(n_chan - 1):
            pj(k * per + i).wait_recv()
            value = value + r.proj_rx[k * per + i].astype(F32)
        r.out[:, i * tile_n : (i + 1) * tile_n] = (inv_mine * value).astype(BF16)

    def all_sent(ref, sem):
        remote(ref, ref, sem, r.fin_recv, partner).wait_send()

    def sums_arrive(n):
        remote(r.fin.at[0:n], r.fin.at[0:n], r.fin_send, r.fin_recv, partner).wait_recv()

    pl.when(dp < root)(lambda: sums_arrive(n_seq))
    pl.when(dp == root)(lambda: sums_arrive(n_seq - 1))
    skip_total = jnp.zeros((8, heads), F32)
    for which in (0, 1):
        final = r.fin[which]
        for k in range(1, n_seq // 2):
            final = final + r.fin[2 * k + which]
        r.gg[:, which * half : (which + 1) * half] = final[0:1, :]
        skip_cols = jnp.concatenate([final[1:2, :], jnp.zeros((7, half), F32)], axis=0)
        for part in split(skip_cols, 3):
            skip_total = skip_total + dot_cols(part, spread_all(which))
    r.gs[...] = skip_total[0:1, :]

    for c in range(chunks):
        send_g(c, other).wait_recv()

    for copy in [send_sm(mine), send_b(mine), send_c(mine), send_z(mine), send_n()]:
        copy.wait_send()
    for copy in do_copies:
        copy.wait_send()
    all_sent(r.stat_rx, r.st_send)
    if sent_tiles:
        all_sent(r.proj_tx, r.pj_send)
    all_sent(r.xo, r.x_send)
    all_sent(r.gtx, r.g_send)
    all_sent(r.ptx, r.pl_send)
    for k in range(root):
        pl.when(dp == k)(red_root(k).wait_send)
    pl.when(dp == root)(lambda: all_sent(r.fin.at[0 : n_seq * n_dp - 1], r.fin_send))
    pl.when(has_prev)(lambda: all_sent(r.txc.at[BWD], r.c_send.at[BWD]))
    pl.when(has_next)(lambda: all_sent(r.txc.at[FWD], r.c_send.at[FWD]))


def hand_over(*refs):
    for source, target in zip(refs[:4], refs[4:]):
        target[...] = source[...]


def local(
    mesh_shape, ssm_input, gate_z, b_proj, c_proj, step_size, log_decay, skip_d, norm_gain, w_out, d_out, game_lengths
):
    n_seq, n_chan, n_dp = (mesh_shape[a] for a in ("seq", "chan", "dp"))
    _, rows, width = ssm_input.shape
    heads = step_size.shape[2]
    states = b_proj.shape[2]
    model = w_out.shape[1]
    nb = d_out.shape[2]
    half = width // 2
    hh = heads // 2
    chunks = max(1, min(8, half // 128))
    cw = half // chunks
    group = 2 if chunks % 2 == 0 else 1
    gw = group * cw
    groups = chunks // group
    peers = max(1, n_chan - 1)
    tile_n = min(256, nb)
    tiles = peers * (nb // tile_n)
    stat_peers = 2 * n_chan - 1
    games = game_lengths.shape[1]
    sizes = (n_seq, n_chan, n_dp, heads, games, chunks, group)
    vmem = pl.BlockSpec(memory_space=pltpu.VMEM)
    hbm = pl.BlockSpec(memory_space=pltpu.HBM)

    def dma(*shape):
        return pltpu.SemaphoreType.DMA(shape)

    inputs = dict(
        x=ssm_input[0],
        b=b_proj[0],
        c=c_proj[0],
        dt=step_size[0].T,
        ld=log_decay[0].T,
        skip=skip_d[None],
        gain=norm_gain[None],
        gl=game_lengths,
        z=gate_z[0],
        w=w_out,
        do=d_out[0],
    )
    outputs = dict(
        out=pltpu.VMEM((rows, nb), BF16),
        gx=pltpu.VMEM((rows, width), BF16),
        gg=pltpu.VMEM((1, width), F32),
        gs=pltpu.VMEM((1, heads), F32),
    )
    both = (2, rows, half)
    scratch = dict(
        xv=pltpu.VMEM((2, chunks, rows, cw), BF16),
        xo=pltpu.VMEM((chunks, rows, cw), BF16),
        zv=pltpu.VMEM(both, BF16),
        zo=pltpu.VMEM((rows, half), BF16),
        bv=pltpu.VMEM((2, rows, states), BF16),
        cv=pltpu.VMEM((2, rows, states), BF16),
        bt=pltpu.VMEM((2, states, rows), BF16),
        ct=pltpu.VMEM((2, states, rows), BF16),
        ldv=pltpu.VMEM((heads, rows), F32),
        smf=pltpu.VMEM((2, heads, rows), F32),
        sm=pltpu.VMEM((2, 2, hh, rows), F32),
        runc=pltpu.VMEM((2, rows, hh), F32),
        skipv=pltpu.VMEM((1, heads), F32),
        gainv=pltpu.VMEM((1, width), F32),
        gls=pltpu.SMEM((1, games), jnp.int32),
        wv=pltpu.VMEM((width, model), BF16),
        dfull=pltpu.VMEM((n_chan, rows, nb), BF16),
        carry_e=pltpu.VMEM(both, F32),
        tdt_e=pltpu.VMEM(both, F32),
        skip_e=pltpu.VMEM((1, half), F32),
        mix=pltpu.VMEM((2, hh // 2, 2 * rows, rows), BF16),
        inside=pltpu.VMEM(both, F32),
        act=pltpu.VMEM(both, F32),
        gated=pltpu.VMEM(both, F32),
        nrm=pltpu.VMEM(both, BF16),
        nrx=pltpu.VMEM((rows, half), BF16),
        d=pltpu.VMEM(both, BF16),
        ptx=pltpu.VMEM((groups, rows, gw), BF16),
        pv=pltpu.VMEM((2, groups, rows, gw), BF16),
        f=pltpu.VMEM((2, chunks, states, cw), F32),
        txc=pltpu.VMEM((2, chunks, states, cw), BF16),
        st=pltpu.VMEM((2, 2, chunks, states, cw), BF16),
        sums=pltpu.VMEM((2, 2, rows, 128), F32),
        invs=pltpu.VMEM((2, rows, 128), F32),
        backs=pltpu.VMEM((2, rows, 128), F32),
        stat_tx=pltpu.VMEM((8, rows), F32),
        stat_rx=pltpu.VMEM((stat_peers, 8, rows), F32),
        proj_tx=pltpu.VMEM((tiles, rows, tile_n), BF16),
        proj_rx=pltpu.VMEM((tiles, rows, tile_n), BF16),
        proj_own=pltpu.VMEM((nb // tile_n, rows, tile_n), F32),
        gtx=pltpu.VMEM((chunks, rows, cw), BF16),
        red_tx=pltpu.VMEM((2, 2, half), F32),
        red_rx=pltpu.VMEM((max(1, n_dp - 1), 2, half), F32),
        fin=pltpu.VMEM((n_seq * n_dp, 2, half), F32),
        load_sem=dma(13),
        p_send=dma(5),
        p_recv=dma(5),
        x_send=pltpu.SemaphoreType.DMA,
        x_recv=dma(chunks),
        pl_send=pltpu.SemaphoreType.DMA,
        pl_recv=dma(groups),
        g_send=pltpu.SemaphoreType.DMA,
        g_recv=dma(chunks),
        c_send=dma(2),
        c_recv=dma(2, chunks),
        do_send=dma(peers),
        do_recv=dma(peers),
        st_send=pltpu.SemaphoreType.DMA,
        st_recv=dma(stat_peers),
        pj_send=pltpu.SemaphoreType.DMA,
        pj_recv=dma(tiles),
        rd_send=dma(1),
        rd_recv=dma(max(1, n_dp - 1)),
        fin_send=pltpu.SemaphoreType.DMA,
        fin_recv=pltpu.SemaphoreType.DMA,
        go=pltpu.SemaphoreType.REGULAR,
        up=pltpu.SemaphoreType.REGULAR,
    )
    names = tuple(inputs) + tuple(outputs) + tuple(scratch)
    results = pl.pallas_call(
        functools.partial(kernel, sizes, names),
        out_shape=tuple(outputs.values()),
        in_specs=[hbm] * len(inputs),
        out_specs=(vmem,) * 4,
        scratch_shapes=list(scratch.values()),
        compiler_params=pltpu.CompilerParams(
            collective_id=0, has_side_effects=True, vmem_limit_bytes=60 * 1024 * 1024
        ),
    )(*inputs.values())
    out, gx, gg, gs = pl.pallas_call(
        hand_over,
        out_shape=tuple(jax.ShapeDtypeStruct(a.shape, a.dtype) for a in results),
        in_specs=[vmem] * 4,
        out_specs=(vmem,) * 4,
        compiler_params=pltpu.CompilerParams(vmem_limit_bytes=4 * 1024 * 1024),
    )(*results)
    return out[None], gx[None], gg[0], gs[0]


def solution(mesh):
    return jax.shard_map(
        functools.partial(local, dict(mesh.shape)),
        mesh=mesh,
        in_specs=(
            P("dp", "seq", "chan"),
            P("dp", "seq", "chan"),
            P("dp", "seq", None),
            P("dp", "seq", None),
            P("dp", "seq", "chan"),
            P("dp", "seq", "chan"),
            P("chan"),
            P("chan"),
            P("chan", None),
            P("dp", "seq", "chan"),
            P("dp", None),
        ),
        out_specs=(P("dp", "seq", "chan"), P("dp", "seq", "chan"), P("chan"), P("chan")),
        check_vma=False,
    )
```

```python
import functools
import types

import jax
import jax.numpy as jnp
from jax import lax
from jax.experimental import pallas as pl
from jax.experimental.pallas import tpu as pltpu
from jax.sharding import PartitionSpec as P

NORM_EPS = 1e-05
F32 = jnp.float32
BF16 = jnp.bfloat16
MESH = pl.DeviceIdType.MESH
FWD, BWD = 0, 1


def dot(a, b):
    return lax.dot_general(a, b, (((1,), (0,)), ((), ())), preferred_element_type=F32)


def dot_rows(a, b):
    return lax.dot_general(a, b, (((0,), (0,)), ((), ())), preferred_element_type=F32)


def dot_cols(a, b):
    return lax.dot_general(a, b, (((1,), (1,)), ((), ())), preferred_element_type=F32)


def split(value, terms):
    parts = []
    for _ in range(terms):
        part = value.astype(BF16)
        parts.append(part)
        value = value - part.astype(F32)
    return parts


def kernel(sizes, names, *refs):
    r = types.SimpleNamespace(**dict(zip(names, refs)))
    n_seq, n_chan, n_dp, heads, games, chunks, group = sizes
    rows, width = r.x.shape
    hd = width // heads
    half = width // 2
    hh = heads // 2
    cw = half // chunks
    gw = group * cw
    groups = chunks // group
    total_width = width * n_chan
    nb = r.out.shape[1]
    seq = lax.axis_index("seq")
    chan = lax.axis_index("chan")
    dp = lax.axis_index("dp")
    mine = lax.rem(seq, 2)
    other = 1 - mine
    pair = seq + 1 - 2 * mine
    partner = {"seq": pair}
    place = seq // 2
    last = n_seq // 2 - 1
    has_prev, has_next = place > 0, place < last
    prev_dev = {"seq": lax.rem(seq + n_seq - 2, n_seq)}
    next_dev = {"seq": lax.rem(seq + 2, n_seq)}

    siblings = [{"dp": lax.rem(dp + k, n_dp)} for k in range(1, n_dp)]
    offs = [lax.rem(chan + off, n_chan) for off in range(1, n_chan)]
    chan_peers = [{"chan": o} for o in offs]
    stat_peers = [partner] + chan_peers + [{"seq": pair, "chan": o} for o in offs]
    greet = [partner] + chan_peers + siblings
    barrier = pltpu.get_barrier_semaphore()

    def hello(peer):
        pl.semaphore_signal(barrier, inc=1, device_id=peer, device_id_type=MESH)

    for peer in greet:
        hello(peer)
    pl.when(has_prev)(lambda: hello(prev_dev))
    pl.when(has_next)(lambda: hello(next_dev))

    my_half = pl.ds(pl.multiple_of(mine * half, half), half)
    other_half = pl.ds(pl.multiple_of(other * half, half), half)
    order = {}

    def load(name, src, dst):
        order[name] = pltpu.make_async_copy(src, dst, r.load_sem.at[len(order)])
        order[name].start()

    def load_chunks(name, which, dst):
        for g in range(groups):
            at = pl.ds(pl.multiple_of(which * half + g * gw, gw), gw)
            pltpu.make_async_copy(r.x.at[:, at], dst.at[g], r.load_sem.at[len(order)]).start()
        order[name] = pltpu.make_async_copy(dst, dst, r.load_sem.at[len(order)])

    load("ld", r.ld, r.ldv)
    load("gl", r.gl, r.gls)
    load("dt", r.dt, r.smf.at[1])
    load("b", r.b, r.bv.at[mine])
    load_chunks("xo", other, r.xo)
    load("do", r.do, r.dfull.at[0])
    load_chunks("x", mine, r.xv.at[mine])
    load("c", r.c, r.cv.at[mine])
    load("skip", r.skip, r.skipv)
    load("zo", r.z.at[:, other_half], r.zo)
    load("z", r.z.at[:, my_half], r.zv.at[mine])
    load("gain", r.gain, r.gainv)
    load("w", r.w, r.wv)

    def remote(src, dst, ssem, rsem, peer):
        return pltpu.make_async_remote_copy(
            src_ref=src, dst_ref=dst, send_sem=ssem, recv_sem=rsem, device_id=peer, device_id_type=MESH
        )

    def ccols(c):
        return pl.ds(pl.multiple_of(c * cw, cw), cw)

    def gcols(g):
        return pl.ds(pl.multiple_of(g * gw, gw), gw)

    def gain_of(g):
        return r.gainv[:, pl.ds(pl.multiple_of(mine * half + g * gw, gw), gw)]

    def send_sm(blk):
        src = r.smf.at[:, pl.ds(pl.multiple_of(other * hh, hh), hh), :]
        return remote(src, r.sm.at[blk], r.p_send.at[0], r.p_recv.at[0], partner)

    def send_b(blk):
        return remote(r.bv.at[blk], r.bv.at[blk], r.p_send.at[1], r.p_recv.at[1], partner)

    def send_c(blk):
        return remote(r.cv.at[blk], r.cv.at[blk], r.p_send.at[2], r.p_recv.at[2], partner)

    def send_z(blk):
        return remote(r.zo, r.zv.at[blk], r.p_send.at[3], r.p_recv.at[3], partner)

    def send_n():
        return remote(r.nrm.at[other], r.nrx, r.p_send.at[4], r.p_recv.at[4], partner)

    def send_x(blk, g):
        return remote(r.xo.at[g], r.xv.at[blk, g], r.x_send, r.x_recv.at[g], partner)

    def send_p(blk, g):
        return remote(r.ptx.at[g], r.pv.at[blk, g], r.pl_send, r.pl_recv.at[g], partner)

    def send_g(g, of):
        at = pl.ds(pl.multiple_of(of * half + g * gw, gw), gw)
        return remote(r.gtx.at[g], r.gx.at[:, at], r.g_send, r.g_recv, partner)

    half_way = n_seq // 4 - 1 if n_seq >= 4 else 0
    spots = (place, last - place)
    early = (dp == 0, dp == n_dp - 1)
    plain_end = tuple(last - e.astype(jnp.int32) for e in early)

    def onward(d):
        return next_dev if d == FWD else prev_dev

    def send_late(d, c):
        return remote(r.txc.at[d, c], r.st.at[d, d, c], r.c_send.at[d], r.c_recv.at[d, c], onward(d))

    def send_early(d, c):
        return remote(r.txe.at[d, c], r.ex.at[d, c], r.e_send.at[d], r.e_recv.at[d, c], onward(d))

    def send_final(d, c):
        return remote(r.txe.at[d, c], r.st.at[d, d, c], r.e_send.at[d], r.c_recv.at[d, c], onward(d))

    do_copies = [
        remote(r.dfull.at[0], r.dfull.at[k + 1], r.do_send.at[k], r.do_recv.at[k], peer)
        for k, peer in enumerate(chan_peers)
    ]

    row_i = lax.broadcasted_iota(jnp.int32, (rows, rows), 0)
    col_i = lax.broadcasted_iota(jnp.int32, (rows, rows), 1)
    causal = row_i >= col_i
    tri = causal.astype(F32).astype(BF16)
    spread = (
        lax.broadcasted_iota(jnp.int32, (hh, half), 1) // hd == lax.broadcasted_iota(jnp.int32, (hh, half), 0)
    ).astype(F32).astype(BF16)

    def spread_all(which):
        at = lax.broadcasted_iota(jnp.int32, (heads, half), 1) // hd + which * hh
        return (at == lax.broadcasted_iota(jnp.int32, (heads, half), 0)).astype(F32).astype(BF16)

    order["ld"].wait()
    running = jnp.zeros((heads, rows), F32)
    for part in split(r.ldv[...], 3):
        running = running + dot_cols(part, tri)
    r.smf[0] = running
    order["gl"].wait()

    def counts(blk):
        base = (2 * place + blk) * rows
        col = jnp.zeros((rows, 1), jnp.int32)
        row = jnp.zeros((1, rows), jnp.int32)
        end = jnp.zeros((1, 1), jnp.int32)
        pos_col = base + lax.broadcasted_iota(jnp.int32, (rows, 1), 0)
        pos_row = base + lax.broadcasted_iota(jnp.int32, (1, rows), 1)
        pos_end = base + rows - 1 + lax.broadcasted_iota(jnp.int32, (1, 1), 0)
        begin = jnp.int32(0)
        for g in range(games):
            here = (begin >= base).astype(jnp.int32)
            col = col + (pos_col >= begin).astype(jnp.int32) * here
            row = row + (pos_row >= begin).astype(jnp.int32) * here
            end = end + (pos_end >= begin).astype(jnp.int32) * here
            begin = begin + r.gls[0, g]
        return col, row, end

    def expand(value, terms):
        total = None
        for part in split(value, terms):
            piece = dot_rows(part, spread)
            total = piece if total is None else total + piece
        return total

    def prepare(blk):
        run = r.sm[blk, 0]
        _, row, end = counts(blk)
        carry = jnp.where(row == 0, jnp.exp(run), 0.0)
        tail = jnp.where(row == end, jnp.exp(run[:, rows - 1 : rows] - run), 0.0)
        r.tdt_e[blk] = expand(tail * r.sm[blk, 1], 2)
        r.carry_e[blk] = expand(carry, 2)
        r.runc[blk] = run.T
        r.bt[blk] = r.bv[blk].T

    my_heads = pl.ds(pl.multiple_of(mine * hh, hh), hh)
    order["dt"].wait()
    order["b"].wait()

    def report():
        pl.semaphore_signal(r.up, inc=1, device_id=prev_dev, device_id_type=MESH)

    def report_up():
        pl.semaphore_signal(r.up, inc=1, device_id=next_dev, device_id_type=MESH)

    def relay():
        pl.semaphore_wait(r.up, 1)
        pl.when(has_prev)(report)

    static = len(greet)
    pl.semaphore_wait(barrier, static + has_prev.astype(jnp.int32) + has_next.astype(jnp.int32))
    pl.when(place == last)(report)
    order["xo"].wait()
    order["do"].wait()
    order["c"].wait()
    order["zo"].wait()

    def first_sends():
        send_sm(mine).start()
        send_b(mine).start()
        for g in range(groups):
            send_x(mine, g).start()
        send_c(mine).start()

    def cotangent_sends():
        for copy in do_copies:
            copy.start()

    def lead_sends():
        first_sends()
        cotangent_sends()

    def gate_sends():
        send_z(mine).start()

    pl.when(dp == 0)(lead_sends)
    pl.when((dp == 0) & (place >= last - 1))(gate_sends)
    r.sm[mine] = r.smf[:, my_heads, :]
    prepare(mine)
    order["x"].wait()

    def x_group(blk, g):
        return r.xv[blk, g].astype(F32)


    def fresh(blk, g):
        cols = gcols(g)
        scaled = (r.tdt_e[blk, :, cols] * x_group(blk, g)).astype(BF16)
        block = dot(r.bt[blk], scaled)
        for k in range(group):
            r.f[blk, g * group + k] = block[:, k * cw : (k + 1) * cw]

    def loop(n, body):
        def step(i, _):
            body(i)
            return 0

        lax.fori_loop(0, n, step, 0)

    loop(groups, lambda g: fresh(mine, g))
    order["skip"].wait()
    skip_pad = jnp.concatenate([r.skipv[...], jnp.zeros((7, heads), F32)], axis=0)
    skip_rows = None
    for part in split(skip_pad, 3):
        piece = dot(part, spread_all(mine))
        skip_rows = piece if skip_rows is None else skip_rows + piece
    r.skip_e[...] = skip_rows[0:1, :]
    pos_lane = lax.broadcasted_iota(jnp.int32, (rows, 2 * hd), 1) < hd

    def block_diag(two):
        two = two.astype(F32)
        return jnp.concatenate(
            [jnp.where(pos_lane, two, 0.0), jnp.where(pos_lane, 0.0, two)], axis=0
        ).astype(BF16)

    def intra(blk):
        col, row, _ = counts(blk)
        r.ct[blk] = r.cv[blk].T
        scores = jnp.where(causal & (col == row), dot_cols(r.cv[blk], r.bv[blk]), 0.0)
        for q in range(hh // 2):
            cols = slice(q * 2 * hd, (q + 1) * 2 * hd)
            mixes = []
            for h in (2 * q, 2 * q + 1):
                gap = jnp.minimum(r.runc[blk, :, h : h + 1] - r.sm[blk, 0, h : h + 1, :], 0.0)
                mixes.append((jnp.exp(gap) * scores * r.sm[blk, 1, h : h + 1, :]).astype(BF16))
                r.mix[blk, q, (h % 2) * rows : (h % 2 + 1) * rows, :] = mixes[-1]
            at = q * 2 * hd
            two = r.xv[blk, at // gw, :, at % gw : at % gw + 2 * hd]
            r.inside[blk, :, cols] = dot(jnp.concatenate(mixes, axis=1), block_diag(two)) + r.skip_e[
                :, cols
            ] * two.astype(F32)

    def silu(blk):
        def body(g):
            zf = r.zv[blk, :, gcols(g)].astype(F32)
            r.act[blk, :, gcols(g)] = zf / (1.0 + jnp.exp(-zf))

        loop(groups, body)

    def dims(d):
        return (0, 1) if d == FWD else (1, 0)

    def through(d, c, mid):
        two = dims(d)[1]
        return (r.carry_e[two, rows - 1 : rows, ccols(c)] * mid + r.f[two, c]).astype(BF16)

    def enter(d, c, state):
        one = dims(d)[0]
        return r.carry_e[one, rows - 1 : rows, ccols(c)] * state.astype(F32) + r.f[one, c]

    def chain(d, c):
        spot = spots[d]

        @pl.when(spot > 0)
        def _():
            send_late(d, c).wait_recv()

        @pl.when(spot == 0)
        def _():
            r.st[d, d, c] = jnp.zeros((r.st.shape[3], cw), BF16)

        mid = enter(d, c, r.st[d, d, c])
        r.st[d, 1 - d, c] = mid.astype(BF16)

        @pl.when(spot < plain_end[d])
        def _():
            r.txc[d, c] = through(d, c, mid)
            send_late(d, c).start()

    def early_start(d, c):
        spot = spots[d]
        r.txe[d, c] = through(d, c, r.f[dims(d)[0], c])
        pl.when(spot == last - 1)(send_final(d, c).start)
        pl.when(spot < last - 1)(send_early(d, c).start)

    def early_pass(d, c):
        spot = spots[d]
        send_early(d, c).wait_recv()
        r.txe[d, c] = through(d, c, enter(d, c, r.ex[d, c]))
        pl.when(spot == last - 1)(send_final(d, c).start)
        pl.when(spot < last - 1)(send_early(d, c).start)

    def starts_early(d):
        return early[d] & (spots[d] == half_way) & (spots[d] < last)

    def passes_early(d):
        return early[d] & (spots[d] > half_way) & (spots[d] < last)

    def meet(g):
        send_x(other, g).wait_recv()
        fresh(other, g)

    def partner_arrives():
        send_sm(other).wait_recv()
        send_b(other).wait_recv()

    def chain_group(d, g):
        for k in range(group):
            chain(d, g * group + k)

    def meet_chain(g):
        meet(g)
        chain_group(FWD, g)

    def early_group(d, g):
        for k in range(group):
            early_start(d, g * group + k)

    def meet_early(g):
        meet(g)
        early_group(FWD, g)

    def own_local():
        intra(mine)
        order["z"].wait()
        silu(mine)

    def late_sends():
        own_local()
        pl.when(place == last - 1)(relay)
        pl.semaphore_wait(r.go, 1)
        lead_sends()
        pl.when(place >= last - 1)(gate_sends)

    def lead_done():
        for k in range(1, n_dp):
            pl.semaphore_signal(r.go, inc=1, device_id={"dp": k}, device_id_type=MESH)

    pl.when(dp > 0)(late_sends)
    partner_arrives()
    pl.when((dp == 0) & (place < last - 1))(lead_done)
    prepare(other)
    pl.when((dp == 0) & (place == last - 1))(relay)

    def pull(lo, hi):
        def body(i, _):
            which = jnp.where(i < groups, other, mine)
            g = lax.rem(i, groups)
            feats = pl.ds(pl.multiple_of(which * half + g * gw, gw), gw)
            total = None
            for k in range(n_chan):
                source = lax.rem(chan + n_chan - k, n_chan)
                piece = dot_cols(r.dfull[k], r.wv[feats, pl.ds(pl.multiple_of(source * nb, nb), nb)])
                total = piece if total is None else total + piece
            value = total.astype(BF16)

            @pl.when(i < groups)
            def _():
                r.ptx[g] = value
                send_p(mine, g).start()

            @pl.when(i >= groups)
            def _():
                r.pv[mine, g] = value

            return 0

        lax.fori_loop(lo, hi, body, 0)

    def pull_ready():
        order["w"].wait()
        for copy in do_copies:
            copy.wait_recv()

    tiles = 2 * groups
    late_place = place >= last - 1

    def pull_first():
        pl.when(dp == 0)(own_local)
        pull_ready()
        pull(0, groups)
        pl.when(dp == 0)(lead_done)

    pl.when(late_place)(pull_first)
    pl.when(place == 0)(lambda: loop(groups, meet_chain))
    pl.when((place > 0) & starts_early(FWD))(lambda: loop(groups, meet_early))
    pl.when((place == 0) & starts_early(FWD))(lambda: loop(groups, lambda g: early_group(FWD, g)))
    pl.when((place > 0) & jnp.logical_not(starts_early(FWD)))(lambda: loop(groups, meet))
    pl.when((place > 0) & (place < last - 1))(relay)
    pl.when((dp == 0) & (place < last - 1))(gate_sends)
    pl.when((dp == 0) & (place < last - 1))(own_local)
    send_c(other).wait_recv()
    intra(other)
    pl.when((dp > 0) & (place < last - 1))(gate_sends)
    pl.when(place == last)(lambda: pull(groups, tiles))
    order["gain"].wait()
    r.sums[...] = jnp.zeros(r.sums.shape, F32)

    def gate(g):
        cols = gcols(g)
        send_p(other, g).wait_recv()
        for blk in (0, 1):
            carried = jnp.concatenate(
                [dot(r.cv[blk], r.st[FWD, blk, g * group + k]) for k in range(group)], axis=1
            )
            gated = (r.inside[blk, :, cols] + r.carry_e[blk, :, cols] * carried) * r.act[blk, :, cols]
            normed = (gated * gain_of(g)).astype(BF16)
            r.gated[blk, :, cols] = gated
            r.nrm[blk, :, cols] = normed
            sq = gated * gated
            od = normed.astype(F32) * r.pv[blk, g].astype(F32)
            squares, dots = r.sums[blk, 0], r.sums[blk, 1]
            for k in range(gw // 128):
                squares = squares + sq[:, k * 128 : (k + 1) * 128]
                dots = dots + od[:, k * 128 : (k + 1) * 128]
            r.sums[blk, 0] = squares
            r.sums[blk, 1] = dots

    def gate_ready():
        send_z(other).wait_recv()
        silu(other)

    def chain_gate(g):
        chain_group(FWD, g)
        gate(g)

    def at_last():
        gate_ready()
        loop(groups, chain_gate)

    def pull_rest():
        pl.when(place < last - 1)(pull_ready)
        pull(jnp.where(place == last - 1, groups, 0), tiles)

    def pass_and_pull():
        loop(chunks, lambda c: early_pass(FWD, c))
        pull_rest()

    def before_last():
        passes = passes_early(FWD)
        pl.when(passes)(pass_and_pull)
        pl.when(place > 0)(lambda: loop(chunks, lambda c: chain(FWD, c)))
        pl.when(place == last - 1)(report_up)
        pl.when(jnp.logical_not(passes))(pull_rest)
        gate_ready()
        loop(groups, gate)

    pl.when(place == last)(at_last)
    pl.when(place < last)(before_last)

    lane = lax.broadcasted_iota(jnp.int32, (rows, 128), 1)
    stats = jnp.zeros((rows, 128), F32)
    for blk in (0, 1):
        for k in (0, 1):
            col = jnp.sum(r.sums[blk, k], axis=1, keepdims=True)
            stats = jnp.where(lane == 2 * blk + k, col, stats)
    r.stat_tx[...] = stats.T[0:8, :]
    st_copies = []
    for k, peer in enumerate(stat_peers):
        st_copies.append(remote(r.stat_tx, r.stat_rx.at[k], r.st_send, r.st_recv, peer))
        st_copies[-1].start()
    lags = (dp == 0) & late_place
    pl.when(jnp.logical_not(lags))(lambda: send_n().start())
    total = r.stat_tx[...]
    remote(r.stat_rx, r.stat_rx, r.st_send, r.st_recv, partner).wait_recv()
    for k in range(len(stat_peers)):
        total = total + r.stat_rx[k]
    stat_cols = jnp.concatenate([total, jnp.zeros((rows - 8, rows), F32)], axis=0).T
    inv, back = [], []
    for blk in (0, 1):
        inv.append(lax.rsqrt(stat_cols[:, 2 * blk : 2 * blk + 1] / total_width + NORM_EPS))
        back.append(inv[blk] * inv[blk] * inv[blk] * stat_cols[:, 2 * blk + 1 : 2 * blk + 2] / total_width)
        r.invs[blk] = jnp.broadcast_to(inv[blk], (rows, 128))
        r.backs[blk] = jnp.broadcast_to(back[blk], (rows, 128))

    def wide(ref, blk):
        return jnp.concatenate([ref[blk]] * (gw // 128), axis=1)

    def cotangent(g):
        cols = gcols(g)
        for blk in (0, 1):
            gated = r.gated[blk, :, cols]
            d_normed = wide(r.invs, blk) * r.pv[blk, g].astype(F32)
            d = ((gain_of(g) * d_normed - wide(r.backs, blk) * gated) * r.act[blk, :, cols]).astype(BF16)
            r.d[blk, :, cols] = d
            weighted = (r.carry_e[blk, :, cols] * d.astype(F32)).astype(BF16)
            block = dot(r.ct[blk], weighted)
            for k in range(group):
                r.f[blk, g * group + k] = block[:, k * cw : (k + 1) * cw]

    def cotangent_chain(g):
        cotangent(g)
        chain_group(BWD, g)

    def cotangent_early(g):
        cotangent(g)
        early_group(BWD, g)

    begins = starts_early(BWD)
    pl.when(place == last)(lambda: loop(groups, cotangent_chain))
    pl.when((place < last) & begins)(lambda: loop(groups, cotangent_early))
    pl.when((place == last) & begins)(lambda: loop(groups, lambda g: early_group(BWD, g)))
    pl.when((place < last) & jnp.logical_not(begins))(lambda: loop(groups, cotangent))

    pl.when(lags)(lambda: send_n().start())

    def terms(g):
        cols = gcols(g)
        gain_sum = skip_sum = None
        for blk in (0, 1):
            a = r.gated[blk, :, cols] * (wide(r.invs, blk) * r.pv[blk, g].astype(F32))
            s = r.d[blk, :, cols].astype(F32) * x_group(blk, g)
            gain_sum = a if gain_sum is None else gain_sum + a
            skip_sum = s if skip_sum is None else skip_sum + s
        r.red_tx[0, 0:1, cols] = jnp.sum(gain_sum, axis=0, keepdims=True)
        r.red_tx[0, 1:2, cols] = jnp.sum(skip_sum, axis=0, keepdims=True)

    loop(groups, terms)

    root = n_dp - 1

    def red_root(k):
        to = {"dp": root}
        return remote(r.red_tx.at[0], r.red_rx.at[k], r.rd_send.at[0], r.rd_recv.at[k], to)

    n_place = n_seq // 2
    along = [{"seq": lax.rem(seq + 2 * k, n_seq)} for k in range(1, n_place)]
    around = [
        {"seq": seq if k == 0 else pair, "dp": lax.rem(dp + j, n_dp)} for k in (0, 1) for j in range(n_dp) if k or j
    ]

    def red_along(where, k):
        return remote(r.red_tx.at[1], r.red_z.at[where], r.fin_send.at[0], r.fin_recv.at[0], along[k])

    def red_around(which, k):
        return remote(r.fin.at[which], r.fin.at[which], r.fin_send.at[1], r.fin_recv.at[1 + which], around[k])

    for k in range(root):
        pl.when(dp == k)(red_root(k).start)

    def spread_sums():
        total = r.red_tx[0]
        for k in range(root):
            red_root(k).wait_recv()
            total = total + r.red_rx[k]
        r.red_tx[1] = total
        r.red_z[place] = total
        for k in range(len(along)):
            red_along(place, k).start()

    def share_sums():
        got = r.red_z.at[0 : n_place - 1]
        remote(got, got, r.fin_send.at[0], r.fin_recv.at[0], partner).wait_recv()
        total = r.red_z[0]
        for k in range(1, n_place):
            total = total + r.red_z[k]
        r.fin[mine] = total
        for k in range(len(around)):
            red_around(mine, k).start()

    def intra_back(blk):
        for q in range(hh // 2):
            cols = slice(q * 2 * hd, (q + 1) * 2 * hd)
            two = r.d[blk, :, cols]
            r.inside[blk, :, cols] = dot_rows(r.mix[blk, q], block_diag(two)) + r.skip_e[:, cols] * two.astype(
                F32
            )

    intra_back(other)
    intra_back(mine)
    pl.when(place == 0)(relay)
    pl.when(place == last)(lambda: pl.semaphore_wait(r.up, 1))
    pl.when(dp == root)(spread_sums)

    tile_n = min(256, nb)
    per = nb // tile_n
    sent_tiles = (n_chan - 1) * per

    def pj(t):
        to = {"chan": lax.rem(chan + 1 + t // per, n_chan)}
        return remote(r.proj_tx.at[t], r.proj_rx.at[t], r.pj_send, r.pj_recv.at[t], to)

    def project(t):
        block = lax.rem(chan + 1 + t // per, n_chan)
        at = pl.ds(pl.multiple_of(block * nb + lax.rem(t, per) * tile_n, tile_n), tile_n)
        value = dot(r.nrm[mine], r.wv[my_half, at]) + dot(r.nrx[...], r.wv[other_half, at])

        @pl.when(t < sent_tiles)
        def _():
            r.proj_tx[t] = value.astype(BF16)
            pj(t).start()

        @pl.when(t >= sent_tiles)
        def _():
            r.proj_own[t - sent_tiles] = value

    n_tiles = sent_tiles + per

    def finish(g):
        cols = gcols(g)

        def value(blk):
            carried = jnp.concatenate([dot(r.bv[blk], r.st[BWD, blk, g * group + k]) for k in range(group)], axis=1)
            return (r.inside[blk, :, cols] + r.tdt_e[blk, :, cols] * carried).astype(BF16)

        theirs, ours = value(other), value(mine)
        r.gtx[g] = theirs
        send_g(g, mine).start()
        r.gx[:, pl.ds(pl.multiple_of(mine * half + g * gw, gw), gw)] = ours

    def chain_finish(g):
        chain_group(BWD, g)
        finish(g)

    def back_first():
        send_n().wait_recv()
        loop(sent_tiles, project)
        chain_finish(0)
        pl.when(dp == root)(share_sums)
        loop(groups - 1, lambda g: chain_finish(1 + g))
        loop(per, lambda t: project(sent_tiles + t))

    def project_all():
        send_n().wait_recv()
        loop(n_tiles, project)

    def pass_and_project():
        loop(chunks, lambda c: early_pass(BWD, c))
        pl.when(dp == root)(share_sums)
        project_all()

    def back_middle():
        passes = passes_early(BWD)
        pl.when(passes)(pass_and_project)
        loop(chunks, lambda c: chain(BWD, c))
        loop(groups, finish)
        pl.when((dp == root) & jnp.logical_not(passes))(share_sums)
        pl.when(jnp.logical_not(passes))(project_all)

    def back_last():
        loop(groups, finish)
        send_n().wait_recv()
        pl.when(dp == root)(share_sums)
        loop(n_tiles, project)

    pl.when(place == 0)(back_first)
    pl.when((place > 0) & (place < last))(back_middle)
    pl.when(place == last)(back_last)
    inv_mine = jnp.concatenate([r.invs[mine]] * (tile_n // 128), axis=1)
    for i in range(per):
        value = r.proj_own[i]
        for k in range(n_chan - 1):
            pj(k * per + i).wait_recv()
            value = value + r.proj_rx[k * per + i].astype(F32)
        r.out[:, i * tile_n : (i + 1) * tile_n] = (inv_mine * value).astype(BF16)

    def all_sent(ref, sem):
        remote(ref, ref, sem, r.fin_recv.at[0], partner).wait_send()

    red_around(other, 0).wait_recv()
    pl.when(dp < root)(lambda: red_around(mine, 0).wait_recv())
    skip_total = jnp.zeros((8, heads), F32)
    for which in (0, 1):
        final = r.fin[which]
        r.gg[:, which * half : (which + 1) * half] = final[0:1, :]
        skip_cols = jnp.concatenate([final[1:2, :], jnp.zeros((7, half), F32)], axis=0)
        for part in split(skip_cols, 3):
            skip_total = skip_total + dot_cols(part, spread_all(which))
    r.gs[...] = skip_total[0:1, :]

    remote(r.gtx, r.gtx, r.g_send, r.g_recv, partner).wait_recv()

    for copy in [send_sm(mine), send_b(mine), send_c(mine), send_z(mine), send_n()]:
        copy.wait_send()
    for copy in do_copies:
        copy.wait_send()
    all_sent(r.stat_rx, r.st_send)
    if sent_tiles:
        all_sent(r.proj_tx, r.pj_send)
    all_sent(r.xo, r.x_send)
    all_sent(r.gtx, r.g_send)
    all_sent(r.ptx, r.pl_send)
    for k in range(root):
        pl.when(dp == k)(red_root(k).wait_send)

    def sums_sent():
        all_sent(r.red_z.at[0 : n_place - 1], r.fin_send.at[0])
        all_sent(r.red_w, r.fin_send.at[1])

    pl.when(dp == root)(sums_sent)
    for d in (FWD, BWD):
        pl.when(spots[d] < plain_end[d])(lambda d=d: all_sent(r.txc.at[d], r.c_send.at[d]))
        pl.when(starts_early(d) | passes_early(d))(lambda d=d: all_sent(r.txe.at[d], r.e_send.at[d]))


def hand_over(*refs):
    sem = refs[8]
    copies = [pltpu.make_async_copy(a, b, sem.at[k]) for k, (a, b) in enumerate(zip(refs[:4], refs[4:8]))]
    for copy in copies:
        copy.start()
    for copy in copies:
        copy.wait()


def local(
    mesh_shape, ssm_input, gate_z, b_proj, c_proj, step_size, log_decay, skip_d, norm_gain, w_out, d_out, game_lengths
):
    n_seq, n_chan, n_dp = (mesh_shape[a] for a in ("seq", "chan", "dp"))
    _, rows, width = ssm_input.shape
    heads = step_size.shape[2]
    states = b_proj.shape[2]
    model = w_out.shape[1]
    nb = d_out.shape[2]
    half = width // 2
    hh = heads // 2
    chunks = max(1, min(8, half // 128))
    cw = half // chunks
    group = 2 if chunks % 2 == 0 else 1
    gw = group * cw
    groups = chunks // group
    peers = max(1, n_chan - 1)
    tile_n = min(256, nb)
    tiles = peers * (nb // tile_n)
    stat_peers = 2 * n_chan - 1
    games = game_lengths.shape[1]
    sizes = (n_seq, n_chan, n_dp, heads, games, chunks, group)
    vmem = pl.BlockSpec(memory_space=pltpu.VMEM)
    hbm = pl.BlockSpec(memory_space=pltpu.HBM)

    def dma(*shape):
        return pltpu.SemaphoreType.DMA(shape)

    inputs = dict(
        x=ssm_input[0],
        b=b_proj[0],
        c=c_proj[0],
        dt=step_size[0].T,
        ld=log_decay[0].T,
        skip=skip_d[None],
        gain=norm_gain[None],
        gl=game_lengths,
        z=gate_z[0],
        w=w_out,
        do=d_out[0],
    )
    outputs = dict(
        out=pltpu.VMEM((rows, nb), BF16),
        gx=pltpu.VMEM((rows, width), BF16),
        gg=pltpu.VMEM((1, width), F32),
        gs=pltpu.VMEM((1, heads), F32),
    )
    both = (2, rows, half)
    scratch = dict(
        xv=pltpu.VMEM((2, groups, rows, gw), BF16),
        xo=pltpu.VMEM((groups, rows, gw), BF16),
        zv=pltpu.VMEM(both, BF16),
        zo=pltpu.VMEM((rows, half), BF16),
        bv=pltpu.VMEM((2, rows, states), BF16),
        cv=pltpu.VMEM((2, rows, states), BF16),
        bt=pltpu.VMEM((2, states, rows), BF16),
        ct=pltpu.VMEM((2, states, rows), BF16),
        ldv=pltpu.VMEM((heads, rows), F32),
        smf=pltpu.VMEM((2, heads, rows), F32),
        sm=pltpu.VMEM((2, 2, hh, rows), F32),
        runc=pltpu.VMEM((2, rows, hh), F32),
        skipv=pltpu.VMEM((1, heads), F32),
        gainv=pltpu.VMEM((1, width), F32),
        gls=pltpu.SMEM((1, games), jnp.int32),
        wv=pltpu.VMEM((width, model), BF16),
        dfull=pltpu.VMEM((n_chan, rows, nb), BF16),
        carry_e=pltpu.VMEM(both, F32),
        tdt_e=pltpu.VMEM(both, F32),
        skip_e=pltpu.VMEM((1, half), F32),
        mix=pltpu.VMEM((2, hh // 2, 2 * rows, rows), BF16),
        inside=pltpu.VMEM(both, F32),
        act=pltpu.VMEM(both, F32),
        gated=pltpu.VMEM(both, F32),
        nrm=pltpu.VMEM(both, BF16),
        nrx=pltpu.VMEM((rows, half), BF16),
        d=pltpu.VMEM(both, BF16),
        ptx=pltpu.VMEM((groups, rows, gw), BF16),
        pv=pltpu.VMEM((2, groups, rows, gw), BF16),
        f=pltpu.VMEM((2, chunks, states, cw), F32),
        txc=pltpu.VMEM((2, chunks, states, cw), BF16),
        txe=pltpu.VMEM((2, chunks, states, cw), BF16),
        ex=pltpu.VMEM((2, chunks, states, cw), BF16),
        st=pltpu.VMEM((2, 2, chunks, states, cw), BF16),
        sums=pltpu.VMEM((2, 2, rows, 128), F32),
        invs=pltpu.VMEM((2, rows, 128), F32),
        backs=pltpu.VMEM((2, rows, 128), F32),
        stat_tx=pltpu.VMEM((8, rows), F32),
        stat_rx=pltpu.VMEM((stat_peers, 8, rows), F32),
        proj_tx=pltpu.VMEM((tiles, rows, tile_n), BF16),
        proj_rx=pltpu.VMEM((tiles, rows, tile_n), BF16),
        proj_own=pltpu.VMEM((nb // tile_n, rows, tile_n), F32),
        gtx=pltpu.VMEM((groups, rows, gw), BF16),
        red_tx=pltpu.VMEM((2, 2, half), F32),
        red_rx=pltpu.VMEM((max(1, n_dp - 1), 2, half), F32),
        red_z=pltpu.VMEM((n_seq // 2, 2, half), F32),
        red_w=pltpu.VMEM((2 * n_dp - 1, 2, half), F32),
        fin=pltpu.VMEM((2, 2, half), F32),
        load_sem=dma(13),
        p_send=dma(5),
        p_recv=dma(5),
        x_send=pltpu.SemaphoreType.DMA,
        x_recv=dma(groups),
        pl_send=pltpu.SemaphoreType.DMA,
        pl_recv=dma(groups),
        g_send=pltpu.SemaphoreType.DMA,
        g_recv=pltpu.SemaphoreType.DMA,
        c_send=dma(2),
        c_recv=dma(2, chunks),
        e_send=dma(2),
        e_recv=dma(2, chunks),
        do_send=dma(peers),
        do_recv=dma(peers),
        st_send=pltpu.SemaphoreType.DMA,
        st_recv=pltpu.SemaphoreType.DMA,
        pj_send=pltpu.SemaphoreType.DMA,
        pj_recv=dma(tiles),
        rd_send=dma(1),
        rd_recv=dma(max(1, n_dp - 1)),
        fin_send=dma(2),
        fin_recv=dma(3),
        go=pltpu.SemaphoreType.REGULAR,
        up=pltpu.SemaphoreType.REGULAR,
    )
    names = tuple(inputs) + tuple(outputs) + tuple(scratch)
    results = pl.pallas_call(
        functools.partial(kernel, sizes, names),
        out_shape=tuple(outputs.values()),
        in_specs=[hbm] * len(inputs),
        out_specs=(vmem,) * 4,
        scratch_shapes=list(scratch.values()),
        compiler_params=pltpu.CompilerParams(
            collective_id=0, has_side_effects=True, vmem_limit_bytes=60 * 1024 * 1024
        ),
    )(*inputs.values())
    out, gx, gg, gs = pl.pallas_call(
        hand_over,
        out_shape=tuple(jax.ShapeDtypeStruct(a.shape, a.dtype) for a in results),
        in_specs=[vmem] * 4,
        out_specs=(hbm,) * 4,
        scratch_shapes=[dma(4)],
        compiler_params=pltpu.CompilerParams(vmem_limit_bytes=4 * 1024 * 1024),
    )(*results)
    return out[None], gx[None], gg[0], gs[0]


def solution(mesh):
    return jax.shard_map(
        functools.partial(local, dict(mesh.shape)),
        mesh=mesh,
        in_specs=(
            P("dp", "seq", "chan"),
            P("dp", "seq", "chan"),
            P("dp", "seq", None),
            P("dp", "seq", None),
            P("dp", "seq", "chan"),
            P("dp", "seq", "chan"),
            P("chan"),
            P("chan"),
            P("chan", None),
            P("dp", "seq", "chan"),
            P("dp", None),
        ),
        out_specs=(P("dp", "seq", "chan"), P("dp", "seq", "chan"), P("chan"), P("chan")),
        check_vma=False,
    )
```

```python
import functools
import types

import jax
import jax.numpy as jnp
from jax import lax
from jax.experimental import pallas as pl
from jax.experimental.pallas import tpu as pltpu
from jax.sharding import PartitionSpec as P

NORM_EPS = 1e-05
F32 = jnp.float32
BF16 = jnp.bfloat16
MESH = pl.DeviceIdType.MESH
FWD, BWD = 0, 1


def dot(a, b):
    return lax.dot_general(a, b, (((1,), (0,)), ((), ())), preferred_element_type=F32)


def dot_rows(a, b):
    return lax.dot_general(a, b, (((0,), (0,)), ((), ())), preferred_element_type=F32)


def dot_cols(a, b):
    return lax.dot_general(a, b, (((1,), (1,)), ((), ())), preferred_element_type=F32)


def split(value, terms):
    parts = []
    for _ in range(terms):
        part = value.astype(BF16)
        parts.append(part)
        value = value - part.astype(F32)
    return parts


def kernel(sizes, names, *refs):
    r = types.SimpleNamespace(**dict(zip(names, refs)))
    n_seq, n_chan, n_dp, heads, games, chunks, group = sizes
    rows, width = r.x.shape
    hd = width // heads
    half = width // 2
    hh = heads // 2
    cw = half // chunks
    gw = group * cw
    groups = chunks // group
    total_width = width * n_chan
    nb = r.out.shape[1]
    seq = lax.axis_index("seq")
    chan = lax.axis_index("chan")
    dp = lax.axis_index("dp")
    mine = lax.rem(seq, 2)
    other = 1 - mine
    pair = seq + 1 - 2 * mine
    partner = {"seq": pair}
    place = seq // 2
    last = n_seq // 2 - 1
    has_prev, has_next = place > 0, place < last
    prev_dev = {"seq": lax.rem(seq + n_seq - 2, n_seq)}
    next_dev = {"seq": lax.rem(seq + 2, n_seq)}

    siblings = [{"dp": lax.rem(dp + k, n_dp)} for k in range(1, n_dp)]
    offs = [lax.rem(chan + off, n_chan) for off in range(1, n_chan)]
    chan_peers = [{"chan": o} for o in offs]
    stat_peers = [partner] + chan_peers + [{"seq": pair, "chan": o} for o in offs]
    greet = [partner] + chan_peers + siblings
    barrier = pltpu.get_barrier_semaphore()

    def hello(peer):
        pl.semaphore_signal(barrier, inc=1, device_id=peer, device_id_type=MESH)

    for peer in greet:
        hello(peer)
    pl.when(has_prev)(lambda: hello(prev_dev))
    pl.when(has_next)(lambda: hello(next_dev))

    my_half = pl.ds(pl.multiple_of(mine * half, half), half)
    other_half = pl.ds(pl.multiple_of(other * half, half), half)
    order = {}

    def load(name, src, dst):
        order[name] = pltpu.make_async_copy(src, dst, r.load_sem.at[len(order)])
        order[name].start()

    def load_chunks(name, which, dst):
        for g in range(groups):
            at = pl.ds(pl.multiple_of(which * half + g * gw, gw), gw)
            pltpu.make_async_copy(r.x.at[:, at], dst.at[g], r.load_sem.at[len(order)]).start()
        order[name] = pltpu.make_async_copy(dst, dst, r.load_sem.at[len(order)])

    load("ld", r.ld, r.ldv)
    load("gl", r.gl, r.gls)
    load("dt", r.dt, r.smf.at[1])
    load("b", r.b, r.bv.at[mine])
    load_chunks("xo", other, r.xo)
    load("do", r.do, r.dfull.at[0])
    load_chunks("x", mine, r.xv.at[mine])
    load("c", r.c, r.cv.at[mine])
    load("skip", r.skip, r.skipv)
    load("zo", r.z.at[:, other_half], r.zo)
    load("z", r.z.at[:, my_half], r.zv.at[mine])
    load("gain", r.gain, r.gainv)
    load("w", r.w, r.wv)

    def remote(src, dst, ssem, rsem, peer):
        return pltpu.make_async_remote_copy(
            src_ref=src, dst_ref=dst, send_sem=ssem, recv_sem=rsem, device_id=peer, device_id_type=MESH
        )

    def ccols(c):
        return pl.ds(pl.multiple_of(c * cw, cw), cw)

    def gcols(g):
        return pl.ds(pl.multiple_of(g * gw, gw), gw)

    def gain_of(g):
        return r.gainv[:, pl.ds(pl.multiple_of(mine * half + g * gw, gw), gw)]

    def send_sm(blk):
        src = r.smf.at[:, pl.ds(pl.multiple_of(other * hh, hh), hh), :]
        return remote(src, r.sm.at[blk], r.p_send.at[0], r.p_recv.at[0], partner)

    def send_b(blk):
        return remote(r.bv.at[blk], r.bv.at[blk], r.p_send.at[1], r.p_recv.at[1], partner)

    def send_c(blk):
        return remote(r.cv.at[blk], r.cv.at[blk], r.p_send.at[2], r.p_recv.at[2], partner)

    def send_z(blk):
        return remote(r.zo, r.zv.at[blk], r.p_send.at[3], r.p_recv.at[3], partner)

    def send_n():
        return remote(r.nrm.at[other], r.nrx, r.p_send.at[4], r.p_recv.at[4], partner)

    def send_x(blk, g):
        return remote(r.xo.at[g], r.xv.at[blk, g], r.x_send, r.x_recv.at[g], partner)

    def send_p(blk, g):
        return remote(r.ptx.at[g], r.pv.at[blk, g], r.pl_send, r.pl_recv.at[g], partner)

    def send_g(g, of):
        at = pl.ds(pl.multiple_of(of * half + g * gw, gw), gw)
        return remote(r.gtx.at[g], r.gx.at[:, at], r.g_send, r.g_recv, partner)

    half_way = n_seq // 4 - 1 if n_seq >= 4 else 0
    spots = (place, last - place)
    early = (dp == 0, dp == n_dp - 1)
    plain_end = tuple(last - e.astype(jnp.int32) for e in early)

    def onward(d):
        return next_dev if d == FWD else prev_dev

    def send_late(d, c):
        return remote(r.txc.at[d, c], r.st.at[d, d, c], r.c_send.at[d], r.c_recv.at[d, c], onward(d))

    def send_early(d, c):
        return remote(r.txe.at[d, c], r.ex.at[d, c], r.e_send.at[d], r.e_recv.at[d, c], onward(d))

    def send_final(d, c):
        return remote(r.txe.at[d, c], r.st.at[d, d, c], r.e_send.at[d], r.c_recv.at[d, c], onward(d))

    do_copies = [
        remote(r.dfull.at[0], r.dfull.at[k + 1], r.do_send.at[k], r.do_recv.at[k], peer)
        for k, peer in enumerate(chan_peers)
    ]

    row_i = lax.broadcasted_iota(jnp.int32, (rows, rows), 0)
    col_i = lax.broadcasted_iota(jnp.int32, (rows, rows), 1)
    causal = row_i >= col_i
    tri = causal.astype(F32).astype(BF16)
    spread = (
        lax.broadcasted_iota(jnp.int32, (hh, half), 1) // hd == lax.broadcasted_iota(jnp.int32, (hh, half), 0)
    ).astype(F32).astype(BF16)

    def spread_all(which):
        at = lax.broadcasted_iota(jnp.int32, (heads, half), 1) // hd + which * hh
        return (at == lax.broadcasted_iota(jnp.int32, (heads, half), 0)).astype(F32).astype(BF16)

    order["ld"].wait()
    running = jnp.zeros((heads, rows), F32)
    for part in split(r.ldv[...], 3):
        running = running + dot_cols(part, tri)
    r.smf[0] = running
    order["gl"].wait()

    def counts(blk):
        base = (2 * place + blk) * rows
        col = jnp.zeros((rows, 1), jnp.int32)
        row = jnp.zeros((1, rows), jnp.int32)
        end = jnp.zeros((1, 1), jnp.int32)
        pos_col = base + lax.broadcasted_iota(jnp.int32, (rows, 1), 0)
        pos_row = base + lax.broadcasted_iota(jnp.int32, (1, rows), 1)
        pos_end = base + rows - 1 + lax.broadcasted_iota(jnp.int32, (1, 1), 0)
        begin = jnp.int32(0)
        for g in range(games):
            here = (begin >= base).astype(jnp.int32)
            col = col + (pos_col >= begin).astype(jnp.int32) * here
            row = row + (pos_row >= begin).astype(jnp.int32) * here
            end = end + (pos_end >= begin).astype(jnp.int32) * here
            begin = begin + r.gls[0, g]
        return col, row, end

    def expand(value, terms):
        total = None
        for part in split(value, terms):
            piece = dot_rows(part, spread)
            total = piece if total is None else total + piece
        return total

    def prepare(blk):
        run = r.sm[blk, 0]
        _, row, end = counts(blk)
        carry = jnp.where(row == 0, jnp.exp(run), 0.0)
        tail = jnp.where(row == end, jnp.exp(run[:, rows - 1 : rows] - run), 0.0)
        r.tdt_e[blk] = expand(tail * r.sm[blk, 1], 2)
        r.carry_e[blk] = expand(carry, 2)
        r.runc[blk] = run.T
        r.bt[blk] = r.bv[blk].T

    my_heads = pl.ds(pl.multiple_of(mine * hh, hh), hh)
    order["dt"].wait()
    order["b"].wait()

    def report():
        pl.semaphore_signal(r.up, inc=1, device_id=prev_dev, device_id_type=MESH)

    def report_up():
        pl.semaphore_signal(r.up, inc=1, device_id=next_dev, device_id_type=MESH)

    def relay():
        pl.semaphore_wait(r.up, 1)
        pl.when(has_prev)(report)

    static = len(greet)
    pl.semaphore_wait(barrier, static + has_prev.astype(jnp.int32) + has_next.astype(jnp.int32))
    pl.when(place == last)(report)
    order["xo"].wait()
    order["do"].wait()
    order["c"].wait()
    order["zo"].wait()

    def first_sends():
        send_sm(mine).start()
        send_b(mine).start()
        for g in range(groups):
            send_x(mine, g).start()
        send_c(mine).start()

    def cotangent_sends():
        for copy in do_copies:
            copy.start()

    def lead_sends():
        first_sends()
        cotangent_sends()

    def gate_sends():
        send_z(mine).start()

    pl.when(dp == 0)(lead_sends)
    pl.when((dp == 0) & (place >= last - 1))(gate_sends)
    r.sm[mine] = r.smf[:, my_heads, :]
    prepare(mine)
    order["x"].wait()

    def x_group(blk, g):
        return r.xv[blk, g].astype(F32)


    def fresh(blk, g):
        cols = gcols(g)
        scaled = (r.tdt_e[blk, :, cols] * x_group(blk, g)).astype(BF16)
        block = dot(r.bt[blk], scaled)
        for k in range(group):
            r.f[blk, g * group + k] = block[:, k * cw : (k + 1) * cw]

    def loop(n, body):
        def step(i, _):
            body(i)
            return 0

        lax.fori_loop(0, n, step, 0)

    loop(groups, lambda g: fresh(mine, g))
    order["skip"].wait()
    skip_pad = jnp.concatenate([r.skipv[...], jnp.zeros((7, heads), F32)], axis=0)
    skip_rows = None
    for part in split(skip_pad, 3):
        piece = dot(part, spread_all(mine))
        skip_rows = piece if skip_rows is None else skip_rows + piece
    r.skip_e[...] = skip_rows[0:1, :]
    pos_lane = lax.broadcasted_iota(jnp.int32, (rows, 2 * hd), 1) < hd

    def block_diag(two):
        two = two.astype(F32)
        return jnp.concatenate(
            [jnp.where(pos_lane, two, 0.0), jnp.where(pos_lane, 0.0, two)], axis=0
        ).astype(BF16)

    def intra(blk):
        col, row, _ = counts(blk)
        r.ct[blk] = r.cv[blk].T
        scores = jnp.where(causal & (col == row), dot_cols(r.cv[blk], r.bv[blk]), 0.0)
        for q in range(hh // 2):
            cols = slice(q * 2 * hd, (q + 1) * 2 * hd)
            mixes = []
            for h in (2 * q, 2 * q + 1):
                gap = jnp.minimum(r.runc[blk, :, h : h + 1] - r.sm[blk, 0, h : h + 1, :], 0.0)
                mixes.append((jnp.exp(gap) * scores * r.sm[blk, 1, h : h + 1, :]).astype(BF16))
                r.mix[blk, q, (h % 2) * rows : (h % 2 + 1) * rows, :] = mixes[-1]
            at = q * 2 * hd
            two = r.xv[blk, at // gw, :, at % gw : at % gw + 2 * hd]
            r.inside[blk, :, cols] = dot(jnp.concatenate(mixes, axis=1), block_diag(two)) + r.skip_e[
                :, cols
            ] * two.astype(F32)

    def silu(blk):
        def body(g):
            zf = r.zv[blk, :, gcols(g)].astype(F32)
            r.act[blk, :, gcols(g)] = zf / (1.0 + jnp.exp(-zf))

        loop(groups, body)

    def dims(d):
        return (0, 1) if d == FWD else (1, 0)

    def through(d, c, mid):
        two = dims(d)[1]
        return (r.carry_e[two, rows - 1 : rows, ccols(c)] * mid + r.f[two, c]).astype(BF16)

    def enter(d, c, state):
        one = dims(d)[0]
        return r.carry_e[one, rows - 1 : rows, ccols(c)] * state.astype(F32) + r.f[one, c]

    def chain(d, c):
        spot = spots[d]

        @pl.when(spot > 0)
        def _():
            send_late(d, c).wait_recv()

        @pl.when(spot == 0)
        def _():
            r.st[d, d, c] = jnp.zeros((r.st.shape[3], cw), BF16)

        mid = enter(d, c, r.st[d, d, c])
        r.st[d, 1 - d, c] = mid.astype(BF16)

        @pl.when(spot < plain_end[d])
        def _():
            r.txc[d, c] = through(d, c, mid)
            send_late(d, c).start()

    def early_start(d, c):
        spot = spots[d]
        r.txe[d, c] = through(d, c, r.f[dims(d)[0], c])
        pl.when(spot == last - 1)(send_final(d, c).start)
        pl.when(spot < last - 1)(send_early(d, c).start)

    def early_pass(d, c):
        spot = spots[d]
        send_early(d, c).wait_recv()
        r.txe[d, c] = through(d, c, enter(d, c, r.ex[d, c]))
        pl.when(spot == last - 1)(send_final(d, c).start)
        pl.when(spot < last - 1)(send_early(d, c).start)

    def starts_early(d):
        return early[d] & (spots[d] == half_way) & (spots[d] < last)

    def passes_early(d):
        return early[d] & (spots[d] > half_way) & (spots[d] < last)

    def meet(g):
        send_x(other, g).wait_recv()
        fresh(other, g)

    def partner_arrives():
        send_sm(other).wait_recv()
        send_b(other).wait_recv()

    def chain_group(d, g):
        for k in range(group):
            chain(d, g * group + k)

    def meet_chain(g):
        meet(g)
        chain_group(FWD, g)

    def early_group(d, g):
        for k in range(group):
            early_start(d, g * group + k)

    def meet_early(g):
        meet(g)
        early_group(FWD, g)

    def own_local():
        intra(mine)
        order["z"].wait()
        silu(mine)

    def late_sends():
        own_local()
        pl.when(place == last - 1)(relay)
        pl.semaphore_wait(r.go, 1)
        lead_sends()
        pl.when(place >= last - 1)(gate_sends)

    def lead_done():
        for k in range(1, n_dp):
            pl.semaphore_signal(r.go, inc=1, device_id={"dp": k}, device_id_type=MESH)

    pl.when(dp > 0)(late_sends)
    partner_arrives()
    pl.when((dp == 0) & (place < last - 1))(lead_done)
    prepare(other)
    pl.when((dp == 0) & (place == last - 1))(relay)

    def pull(lo, hi):
        def body(i, _):
            which = jnp.where(i < groups, other, mine)
            g = lax.rem(i, groups)
            feats = pl.ds(pl.multiple_of(which * half + g * gw, gw), gw)
            total = None
            for k in range(n_chan):
                source = lax.rem(chan + n_chan - k, n_chan)
                piece = dot_cols(r.dfull[k], r.wv[feats, pl.ds(pl.multiple_of(source * nb, nb), nb)])
                total = piece if total is None else total + piece
            value = total.astype(BF16)

            @pl.when(i < groups)
            def _():
                r.ptx[g] = value
                send_p(mine, g).start()

            @pl.when(i >= groups)
            def _():
                r.pv[mine, g] = value

            return 0

        lax.fori_loop(lo, hi, body, 0)

    def pull_ready():
        order["w"].wait()
        for copy in do_copies:
            copy.wait_recv()

    tiles = 2 * groups
    late_place = place >= last - 1

    def pull_first():
        pl.when(dp == 0)(own_local)
        pull_ready()
        pull(0, groups)
        pl.when(dp == 0)(lead_done)

    pl.when(late_place)(pull_first)
    pl.when(place == 0)(lambda: loop(groups, meet_chain))
    pl.when((place > 0) & starts_early(FWD))(lambda: loop(groups, meet_early))
    pl.when((place == 0) & starts_early(FWD))(lambda: loop(groups, lambda g: early_group(FWD, g)))
    pl.when((place > 0) & jnp.logical_not(starts_early(FWD)))(lambda: loop(groups, meet))
    pl.when((place > 0) & (place < last - 1))(relay)
    pl.when((dp == 0) & (place < last - 1))(gate_sends)
    pl.when((dp == 0) & (place < last - 1))(own_local)
    send_c(other).wait_recv()
    intra(other)
    pl.when((dp > 0) & (place < last - 1))(gate_sends)
    pl.when(place == last)(lambda: pull(groups, tiles))
    order["gain"].wait()
    r.sums[...] = jnp.zeros(r.sums.shape, F32)

    def gate(g):
        cols = gcols(g)
        for blk in (0, 1):
            carried = jnp.concatenate(
                [dot(r.cv[blk], r.st[FWD, blk, g * group + k]) for k in range(group)], axis=1
            )
            gated = (r.inside[blk, :, cols] + r.carry_e[blk, :, cols] * carried) * r.act[blk, :, cols]
            normed = (gated * gain_of(g)).astype(BF16)
            r.gated[blk, :, cols] = gated
            r.nrm[blk, :, cols] = normed
            sq = gated * gated
            squares = r.sums[blk, 0]
            for k in range(gw // 128):
                squares = squares + sq[:, k * 128 : (k + 1) * 128]
            r.sums[blk, 0] = squares

    def gate_dots(g):
        send_p(other, g).wait_recv()
        for blk in (0, 1):
            od = r.nrm[blk, :, gcols(g)].astype(F32) * r.pv[blk, g].astype(F32)
            dots = r.sums[blk, 1]
            for k in range(gw // 128):
                dots = dots + od[:, k * 128 : (k + 1) * 128]
            r.sums[blk, 1] = dots

    def gate_ready():
        send_z(other).wait_recv()
        silu(other)

    def chain_gate(g):
        chain_group(FWD, g)
        gate(g)

    def at_last():
        gate_ready()
        loop(groups, chain_gate)
        loop(groups, gate_dots)

    def pull_rest():
        pl.when(place < last - 1)(pull_ready)
        pull(jnp.where(place == last - 1, groups, 0), tiles)

    def pass_and_pull():
        loop(chunks, lambda c: early_pass(FWD, c))
        pull_rest()

    def before_last():
        passes = passes_early(FWD)
        pl.when(passes)(pass_and_pull)
        pl.when(place > 0)(lambda: loop(chunks, lambda c: chain(FWD, c)))
        pl.when(place == last - 1)(report_up)
        pl.when(jnp.logical_not(passes))(pull_rest)
        gate_ready()
        loop(groups, gate)
        loop(groups, gate_dots)

    pl.when(place == last)(at_last)
    pl.when(place < last)(before_last)

    lane = lax.broadcasted_iota(jnp.int32, (rows, 128), 1)
    stats = jnp.zeros((rows, 128), F32)
    for blk in (0, 1):
        for k in (0, 1):
            col = jnp.sum(r.sums[blk, k], axis=1, keepdims=True)
            stats = jnp.where(lane == 2 * blk + k, col, stats)
    r.stat_tx[...] = stats.T[0:8, :]
    st_copies = []
    for k, peer in enumerate(stat_peers):
        st_copies.append(remote(r.stat_tx, r.stat_rx.at[k], r.st_send, r.st_recv, peer))
        st_copies[-1].start()
    lags = (dp == 0) & late_place
    pl.when(jnp.logical_not(lags))(lambda: send_n().start())
    total = r.stat_tx[...]
    remote(r.stat_rx, r.stat_rx, r.st_send, r.st_recv, partner).wait_recv()
    for k in range(len(stat_peers)):
        total = total + r.stat_rx[k]
    stat_cols = jnp.concatenate([total, jnp.zeros((rows - 8, rows), F32)], axis=0).T
    inv, back = [], []
    for blk in (0, 1):
        inv.append(lax.rsqrt(stat_cols[:, 2 * blk : 2 * blk + 1] / total_width + NORM_EPS))
        back.append(inv[blk] * inv[blk] * inv[blk] * stat_cols[:, 2 * blk + 1 : 2 * blk + 2] / total_width)
        r.invs[blk] = jnp.broadcast_to(inv[blk], (rows, 128))
        r.backs[blk] = jnp.broadcast_to(back[blk], (rows, 128))

    def wide(ref, blk):
        return jnp.concatenate([ref[blk]] * (gw // 128), axis=1)

    def cotangent(g):
        cols = gcols(g)
        for blk in (0, 1):
            gated = r.gated[blk, :, cols]
            d_normed = wide(r.invs, blk) * r.pv[blk, g].astype(F32)
            d = ((gain_of(g) * d_normed - wide(r.backs, blk) * gated) * r.act[blk, :, cols]).astype(BF16)
            r.d[blk, :, cols] = d
            weighted = (r.carry_e[blk, :, cols] * d.astype(F32)).astype(BF16)
            block = dot(r.ct[blk], weighted)
            for k in range(group):
                r.f[blk, g * group + k] = block[:, k * cw : (k + 1) * cw]

    def cotangent_chain(g):
        cotangent(g)
        chain_group(BWD, g)

    def cotangent_early(g):
        cotangent(g)
        early_group(BWD, g)

    begins = starts_early(BWD)
    pl.when(place == last)(lambda: loop(groups, cotangent_chain))
    pl.when((place < last) & begins)(lambda: loop(groups, cotangent_early))
    pl.when((place == last) & begins)(lambda: loop(groups, lambda g: early_group(BWD, g)))
    pl.when((place < last) & jnp.logical_not(begins))(lambda: loop(groups, cotangent))

    pl.when(lags)(lambda: send_n().start())

    def terms(g):
        cols = gcols(g)
        gain_sum = skip_sum = None
        for blk in (0, 1):
            a = r.gated[blk, :, cols] * (wide(r.invs, blk) * r.pv[blk, g].astype(F32))
            s = r.d[blk, :, cols].astype(F32) * x_group(blk, g)
            gain_sum = a if gain_sum is None else gain_sum + a
            skip_sum = s if skip_sum is None else skip_sum + s
        r.red_tx[0, 0:1, cols] = jnp.sum(gain_sum, axis=0, keepdims=True)
        r.red_tx[0, 1:2, cols] = jnp.sum(skip_sum, axis=0, keepdims=True)

    loop(groups, terms)

    root = n_dp - 1

    def red_root(k):
        to = {"dp": root}
        return remote(r.red_tx.at[0], r.red_rx.at[k], r.rd_send.at[0], r.rd_recv.at[k], to)

    n_place = n_seq // 2
    along = [{"seq": lax.rem(seq + 2 * k, n_seq)} for k in range(1, n_place)]
    around = [
        {"seq": seq if k == 0 else pair, "dp": lax.rem(dp + j, n_dp)} for k in (0, 1) for j in range(n_dp) if k or j
    ]

    def red_along(where, k):
        return remote(r.red_tx.at[1], r.red_z.at[where], r.fin_send.at[0], r.fin_recv.at[0], along[k])

    def red_around(which, k):
        return remote(r.fin.at[which], r.fin.at[which], r.fin_send.at[1], r.fin_recv.at[1 + which], around[k])

    for k in range(root):
        pl.when(dp == k)(red_root(k).start)

    def spread_sums():
        total = r.red_tx[0]
        for k in range(root):
            red_root(k).wait_recv()
            total = total + r.red_rx[k]
        r.red_tx[1] = total
        r.red_z[place] = total
        for k in range(len(along)):
            red_along(place, k).start()

    def share_sums():
        got = r.red_z.at[0 : n_place - 1]
        remote(got, got, r.fin_send.at[0], r.fin_recv.at[0], partner).wait_recv()
        total = r.red_z[0]
        for k in range(1, n_place):
            total = total + r.red_z[k]
        r.fin[mine] = total
        for k in range(len(around)):
            red_around(mine, k).start()

    def intra_back(blk):
        for q in range(hh // 2):
            cols = slice(q * 2 * hd, (q + 1) * 2 * hd)
            two = r.d[blk, :, cols]
            r.inside[blk, :, cols] = dot_rows(r.mix[blk, q], block_diag(two)) + r.skip_e[:, cols] * two.astype(
                F32
            )

    intra_back(other)
    intra_back(mine)
    pl.when(place == 0)(relay)
    pl.when(place == last)(lambda: pl.semaphore_wait(r.up, 1))
    pl.when(dp == root)(spread_sums)

    tile_n = min(256, nb)
    per = nb // tile_n
    sent_tiles = (n_chan - 1) * per

    def pj(t):
        to = {"chan": lax.rem(chan + 1 + t // per, n_chan)}
        return remote(r.proj_tx.at[t], r.proj_rx.at[t], r.pj_send, r.pj_recv.at[t], to)

    def project(t):
        block = lax.rem(chan + 1 + t // per, n_chan)
        at = pl.ds(pl.multiple_of(block * nb + lax.rem(t, per) * tile_n, tile_n), tile_n)
        value = dot(r.nrm[mine], r.wv[my_half, at]) + dot(r.nrx[...], r.wv[other_half, at])

        @pl.when(t < sent_tiles)
        def _():
            r.proj_tx[t] = value.astype(BF16)
            pj(t).start()

        @pl.when(t >= sent_tiles)
        def _():
            r.proj_own[t - sent_tiles] = value

    n_tiles = sent_tiles + per

    def finish(g):
        cols = gcols(g)

        def value(blk):
            carried = jnp.concatenate([dot(r.bv[blk], r.st[BWD, blk, g * group + k]) for k in range(group)], axis=1)
            return (r.inside[blk, :, cols] + r.tdt_e[blk, :, cols] * carried).astype(BF16)

        theirs, ours = value(other), value(mine)
        r.gtx[g] = theirs
        send_g(g, mine).start()
        r.gx[:, pl.ds(pl.multiple_of(mine * half + g * gw, gw), gw)] = ours

    def finish_chunk(c):
        cols = ccols(c)
        g, k = c // group, c % group

        def value(blk):
            carried = dot(r.bv[blk], r.st[BWD, blk, c])
            return (r.inside[blk, :, cols] + r.tdt_e[blk, :, cols] * carried).astype(BF16)

        def at(of):
            return pl.ds(pl.multiple_of(of * half + c * cw, cw), cw)

        piece = r.gtx.at[g, :, k * cw : (k + 1) * cw]
        r.gtx[g, :, k * cw : (k + 1) * cw] = value(other)
        remote(piece, r.gx.at[:, at(mine)], r.g_send, r.g_recv, partner).start()
        r.gx[:, at(mine)] = value(mine)

    def chain_finish(g):
        chain_group(BWD, g)
        finish(g)

    def back_first():
        send_n().wait_recv()
        loop(sent_tiles, project)
        chain_finish(0)
        pl.when(dp == root)(share_sums)
        loop(max(0, groups - 2), lambda g: chain_finish(1 + g))
        if groups > 1:
            for c in range(chunks - group, chunks):
                chain(BWD, c)
                finish_chunk(c)
        loop(per, lambda t: project(sent_tiles + t))

    def project_all():
        send_n().wait_recv()
        loop(n_tiles, project)

    def pass_and_project():
        loop(chunks, lambda c: early_pass(BWD, c))
        pl.when(dp == root)(share_sums)
        project_all()

    def back_middle():
        passes = passes_early(BWD)
        pl.when(passes)(pass_and_project)
        loop(chunks, lambda c: chain(BWD, c))
        loop(groups, finish)
        pl.when((dp == root) & jnp.logical_not(passes))(share_sums)
        pl.when(jnp.logical_not(passes))(project_all)

    def back_last():
        loop(groups, finish)
        send_n().wait_recv()
        pl.when(dp == root)(share_sums)
        loop(n_tiles, project)

    pl.when(place == 0)(back_first)
    pl.when((place > 0) & (place < last))(back_middle)
    pl.when(place == last)(back_last)
    inv_mine = jnp.concatenate([r.invs[mine]] * (tile_n // 128), axis=1)
    for i in range(per):
        value = r.proj_own[i]
        for k in range(n_chan - 1):
            pj(k * per + i).wait_recv()
            value = value + r.proj_rx[k * per + i].astype(F32)
        r.out[:, i * tile_n : (i + 1) * tile_n] = (inv_mine * value).astype(BF16)

    def all_sent(ref, sem):
        remote(ref, ref, sem, r.fin_recv.at[0], partner).wait_send()

    red_around(other, 0).wait_recv()
    pl.when(dp < root)(lambda: red_around(mine, 0).wait_recv())
    skip_total = jnp.zeros((8, heads), F32)
    for which in (0, 1):
        final = r.fin[which]
        r.gg[:, which * half : (which + 1) * half] = final[0:1, :]
        skip_cols = jnp.concatenate([final[1:2, :], jnp.zeros((7, half), F32)], axis=0)
        for part in split(skip_cols, 3):
            skip_total = skip_total + dot_cols(part, spread_all(which))
    r.gs[...] = skip_total[0:1, :]

    remote(r.gtx, r.gtx, r.g_send, r.g_recv, partner).wait_recv()

    for copy in [send_sm(mine), send_b(mine), send_c(mine), send_z(mine), send_n()]:
        copy.wait_send()
    for copy in do_copies:
        copy.wait_send()
    all_sent(r.stat_rx, r.st_send)
    if sent_tiles:
        all_sent(r.proj_tx, r.pj_send)
    all_sent(r.xo, r.x_send)
    all_sent(r.gtx, r.g_send)
    all_sent(r.ptx, r.pl_send)
    for k in range(root):
        pl.when(dp == k)(red_root(k).wait_send)

    def sums_sent():
        all_sent(r.red_z.at[0 : n_place - 1], r.fin_send.at[0])
        all_sent(r.red_w, r.fin_send.at[1])

    pl.when(dp == root)(sums_sent)
    for d in (FWD, BWD):
        pl.when(spots[d] < plain_end[d])(lambda d=d: all_sent(r.txc.at[d], r.c_send.at[d]))
        pl.when(starts_early(d) | passes_early(d))(lambda d=d: all_sent(r.txe.at[d], r.e_send.at[d]))


def hand_over(*refs):
    sem = refs[8]
    copies = [pltpu.make_async_copy(a, b, sem.at[k]) for k, (a, b) in enumerate(zip(refs[:4], refs[4:8]))]
    for copy in copies:
        copy.start()
    for copy in copies:
        copy.wait()


def local(
    mesh_shape, ssm_input, gate_z, b_proj, c_proj, step_size, log_decay, skip_d, norm_gain, w_out, d_out, game_lengths
):
    n_seq, n_chan, n_dp = (mesh_shape[a] for a in ("seq", "chan", "dp"))
    _, rows, width = ssm_input.shape
    heads = step_size.shape[2]
    states = b_proj.shape[2]
    model = w_out.shape[1]
    nb = d_out.shape[2]
    half = width // 2
    hh = heads // 2
    chunks = max(1, min(8, half // 128))
    cw = half // chunks
    group = 2 if chunks % 2 == 0 else 1
    gw = group * cw
    groups = chunks // group
    peers = max(1, n_chan - 1)
    tile_n = min(256, nb)
    tiles = peers * (nb // tile_n)
    stat_peers = 2 * n_chan - 1
    games = game_lengths.shape[1]
    sizes = (n_seq, n_chan, n_dp, heads, games, chunks, group)
    vmem = pl.BlockSpec(memory_space=pltpu.VMEM)
    hbm = pl.BlockSpec(memory_space=pltpu.HBM)

    def dma(*shape):
        return pltpu.SemaphoreType.DMA(shape)

    inputs = dict(
        x=ssm_input[0],
        b=b_proj[0],
        c=c_proj[0],
        dt=step_size[0].T,
        ld=log_decay[0].T,
        skip=skip_d[None],
        gain=norm_gain[None],
        gl=game_lengths,
        z=gate_z[0],
        w=w_out,
        do=d_out[0],
    )
    outputs = dict(
        out=pltpu.VMEM((rows, nb), BF16),
        gx=pltpu.VMEM((rows, width), BF16),
        gg=pltpu.VMEM((1, width), F32),
        gs=pltpu.VMEM((1, heads), F32),
    )
    both = (2, rows, half)
    scratch = dict(
        xv=pltpu.VMEM((2, groups, rows, gw), BF16),
        xo=pltpu.VMEM((groups, rows, gw), BF16),
        zv=pltpu.VMEM(both, BF16),
        zo=pltpu.VMEM((rows, half), BF16),
        bv=pltpu.VMEM((2, rows, states), BF16),
        cv=pltpu.VMEM((2, rows, states), BF16),
        bt=pltpu.VMEM((2, states, rows), BF16),
        ct=pltpu.VMEM((2, states, rows), BF16),
        ldv=pltpu.VMEM((heads, rows), F32),
        smf=pltpu.VMEM((2, heads, rows), F32),
        sm=pltpu.VMEM((2, 2, hh, rows), F32),
        runc=pltpu.VMEM((2, rows, hh), F32),
        skipv=pltpu.VMEM((1, heads), F32),
        gainv=pltpu.VMEM((1, width), F32),
        gls=pltpu.SMEM((1, games), jnp.int32),
        wv=pltpu.VMEM((width, model), BF16),
        dfull=pltpu.VMEM((n_chan, rows, nb), BF16),
        carry_e=pltpu.VMEM(both, F32),
        tdt_e=pltpu.VMEM(both, F32),
        skip_e=pltpu.VMEM((1, half), F32),
        mix=pltpu.VMEM((2, hh // 2, 2 * rows, rows), BF16),
        inside=pltpu.VMEM(both, F32),
        act=pltpu.VMEM(both, F32),
        gated=pltpu.VMEM(both, F32),
        nrm=pltpu.VMEM(both, BF16),
        nrx=pltpu.VMEM((rows, half), BF16),
        d=pltpu.VMEM(both, BF16),
        ptx=pltpu.VMEM((groups, rows, gw), BF16),
        pv=pltpu.VMEM((2, groups, rows, gw), BF16),
        f=pltpu.VMEM((2, chunks, states, cw), F32),
        txc=pltpu.VMEM((2, chunks, states, cw), BF16),
        txe=pltpu.VMEM((2, chunks, states, cw), BF16),
        ex=pltpu.VMEM((2, chunks, states, cw), BF16),
        st=pltpu.VMEM((2, 2, chunks, states, cw), BF16),
        sums=pltpu.VMEM((2, 2, rows, 128), F32),
        invs=pltpu.VMEM((2, rows, 128), F32),
        backs=pltpu.VMEM((2, rows, 128), F32),
        stat_tx=pltpu.VMEM((8, rows), F32),
        stat_rx=pltpu.VMEM((stat_peers, 8, rows), F32),
        proj_tx=pltpu.VMEM((tiles, rows, tile_n), BF16),
        proj_rx=pltpu.VMEM((tiles, rows, tile_n), BF16),
        proj_own=pltpu.VMEM((nb // tile_n, rows, tile_n), F32),
        gtx=pltpu.VMEM((groups, rows, gw), BF16),
        red_tx=pltpu.VMEM((2, 2, half), F32),
        red_rx=pltpu.VMEM((max(1, n_dp - 1), 2, half), F32),
        red_z=pltpu.VMEM((n_seq // 2, 2, half), F32),
        red_w=pltpu.VMEM((2 * n_dp - 1, 2, half), F32),
        fin=pltpu.VMEM((2, 2, half), F32),
        load_sem=dma(13),
        p_send=dma(5),
        p_recv=dma(5),
        x_send=pltpu.SemaphoreType.DMA,
        x_recv=dma(groups),
        pl_send=pltpu.SemaphoreType.DMA,
        pl_recv=dma(groups),
        g_send=pltpu.SemaphoreType.DMA,
        g_recv=pltpu.SemaphoreType.DMA,
        c_send=dma(2),
        c_recv=dma(2, chunks),
        e_send=dma(2),
        e_recv=dma(2, chunks),
        do_send=dma(peers),
        do_recv=dma(peers),
        st_send=pltpu.SemaphoreType.DMA,
        st_recv=pltpu.SemaphoreType.DMA,
        pj_send=pltpu.SemaphoreType.DMA,
        pj_recv=dma(tiles),
        rd_send=dma(1),
        rd_recv=dma(max(1, n_dp - 1)),
        fin_send=dma(2),
        fin_recv=dma(3),
        go=pltpu.SemaphoreType.REGULAR,
        up=pltpu.SemaphoreType.REGULAR,
    )
    names = tuple(inputs) + tuple(outputs) + tuple(scratch)
    results = pl.pallas_call(
        functools.partial(kernel, sizes, names),
        out_shape=tuple(outputs.values()),
        in_specs=[hbm] * len(inputs),
        out_specs=(vmem,) * 4,
        scratch_shapes=list(scratch.values()),
        compiler_params=pltpu.CompilerParams(
            collective_id=0, has_side_effects=True, vmem_limit_bytes=60 * 1024 * 1024
        ),
    )(*inputs.values())
    out, gx, gg, gs = pl.pallas_call(
        hand_over,
        out_shape=tuple(jax.ShapeDtypeStruct(a.shape, a.dtype) for a in results),
        in_specs=[vmem] * 4,
        out_specs=(hbm,) * 4,
        scratch_shapes=[dma(4)],
        compiler_params=pltpu.CompilerParams(vmem_limit_bytes=4 * 1024 * 1024),
    )(*results)
    return out[None], gx[None], gg[0], gs[0]


def solution(mesh):
    return jax.shard_map(
        functools.partial(local, dict(mesh.shape)),
        mesh=mesh,
        in_specs=(
            P("dp", "seq", "chan"),
            P("dp", "seq", "chan"),
            P("dp", "seq", None),
            P("dp", "seq", None),
            P("dp", "seq", "chan"),
            P("dp", "seq", "chan"),
            P("chan"),
            P("chan"),
            P("chan", None),
            P("dp", "seq", "chan"),
            P("dp", None),
        ),
        out_specs=(P("dp", "seq", "chan"), P("dp", "seq", "chan"), P("chan"), P("chan")),
        check_vma=False,
    )
```
